256 devices in a mesh: cls: 128 (over y, z, x), rep: 2 (over core).
Axes of the slice: x: 4, y: 4, z: 8, core: 2. Of those that a mesh axis runs over, the one named last changes fastest.
Arguments:
- queries: bfloat16 [2, 256, 768], P('rep', 'cls'), may hold values from -16 to 16
- positives: int32 [2, 256, 4], replicated, may hold values from -1 to 786431, as said below
- label_vectors: bfloat16 [786432, 768], P('cls'), may hold values from -80 to 80
- refresh_slot: int32 [], replicated, may hold values from 0 to 7
- features: bfloat16 [98304, 768], P(('cls', 'rep')), may hold values from -6 to 6
- encoder_weight: bfloat16 [768, 768], replicated, may hold values from -0.21875 to 0.21875
- encoder_gain: float32 [768], replicated, may hold values from 0.1 to 1.9
- free_vectors: bfloat16 [98304, 768], P(('cls', 'rep')), may hold values from -3 to 3
- targets: int32 [98304], replicated, may hold values from 0 to 98303, as said below
Outputs:
- loss: float32 [2, 256], P('rep', 'cls')
- query_grads: bfloat16 [2, 256, 768], P('rep', 'cls')
- refreshed_vectors: bfloat16 [98304, 768], P(('cls', 'rep'))
The draws below stay inside these ranges and needn't reach their ends.
Inputs may be any that keep to these rules, and one draw needn't show every extreme that they name: `positives`: each row holds 1 to 4 label ids in its first places and -1 in the rest; ids may repeat within a row. `targets`: A permutation. Refreshed row t belongs to owner t // 768. The b-th aligned block of 384 entries names exactly 3 rows of every owner, all in the half b % 2 of that owner's 768 rows.
All inputs are finite; a program needn't handle non-finite values.
Results may differ from the reference program's by a relative error of at most 0.0048.
Values may be sent and summed in bfloat16 or wider, within the bound.
No kernel may reach another device: no remote copies, remote signals or barrier semaphores. Data moves between devices by JAX's collectives and lax.ppermute only.
A program may use at most 128 MiB of HBM per device.

```python
import jax
import jax.numpy as jnp
from jax import lax

D = 768
LAB_DEV = 6144
SLOTS = 8
POS = 4
Q_DEV = 2
LABELS = 786432
R_DEV = 768
REFRESH = 98304
QG = 256
N_CLS = 128
N_REP = 2


def label_rows(key, row_ids):
    row_base = jax.random.fold_in(key, 11)

    def one_row(row_id):
        return jax.random.normal(jax.random.fold_in(row_base, row_id), (D,), jnp.float32)
    values = jnp.clip(jax.vmap(one_row)(row_ids), -6.0, 6.0)
    return values


def draw_label_vectors(key, part):
    return label_rows(key, jnp.arange(LABELS, dtype=jnp.int32)).astype(jnp.bfloat16)


def draw_queries(key, part):
    total_rows = N_REP * Q_DEV * N_CLS
    spread = 3.0 * D ** (-0.5)
    values = spread * jnp.clip(jax.random.normal(jax.random.fold_in(key, 21), (total_rows, D), jnp.float32), -6.0, 6.0)
    return values.reshape(N_REP, Q_DEV * N_CLS, D).astype(jnp.bfloat16)


def draw_positives(key, part):
    total_rows = N_REP * Q_DEV * N_CLS
    counts = jax.random.randint(jax.random.fold_in(key, 31), (total_rows,), 1, POS + 1)
    counts = counts.at[0].set(POS).at[1].set(1)
    label_ids = jax.random.randint(jax.random.fold_in(key, 32), (total_rows, POS), 0, LABELS)
    places = jnp.arange(POS, dtype=jnp.int32)[None, :]
    filled = jnp.where(places < counts[:, None], label_ids, -1)
    return filled.reshape(N_REP, Q_DEV * N_CLS, POS).astype(jnp.int32)


def draw_targets(key, part):
    half_rows = LAB_DEV // SLOTS // N_REP
    per_owner = half_rows // N_CLS
    key_list = jax.random.split(jax.random.fold_in(key, 41), N_REP * N_CLS)
    shuffled = jax.vmap(lambda one_key: jax.random.permutation(one_key, half_rows))(key_list)
    shuffled = shuffled.reshape(N_REP, N_CLS, N_CLS, per_owner)
    owners = jnp.arange(N_CLS, dtype=jnp.int32)[None, :, None, None]
    halves = jnp.arange(N_REP, dtype=jnp.int32)[:, None, None, None]
    rows_all = owners * (half_rows * N_REP) + halves * half_rows + shuffled
    rows_all = rows_all.transpose(2, 0, 1, 3).reshape(N_CLS * N_REP, N_CLS * per_owner)
    order_keys = jax.random.split(jax.random.fold_in(key, 42), N_CLS * N_REP)
    orders = jax.vmap(lambda one_key: jax.random.permutation(one_key, N_CLS * per_owner))(order_keys)
    rows_all = jnp.take_along_axis(rows_all, orders, axis=1)
    return rows_all.reshape(-1).astype(jnp.int32)


def block_levels(key, extent, cuts, low, top_value):
    def one(dim, shards_of):
        heights = jax.random.uniform(jax.random.fold_in(jax.random.fold_in(key, 6), dim), (shards_of,), jnp.float32, low / len(cuts), top_value / len(cuts))
        return jnp.repeat(jnp.exp(heights), extent[dim] // shards_of).reshape((-1,) + (1,) * (len(extent) - dim - 1))

    factor_of = one(*cuts[0])
    for cut in cuts[1:]:
        factor_of = factor_of * one(*cut)
    return factor_of


def normal_values(key, shape, width, limit, cuts=(), held_as=jnp.bfloat16):
    loudness = block_levels(key, shape, cuts, -0.22, 0.18) if cuts else 1.0
    values = jax.random.normal(key, shape, jnp.float32) * width * loudness
    return jnp.minimum(jnp.maximum(values, -limit), limit).astype(held_as)


def setup_inputs(seed: int = 0) -> dict:
    key_of = jax.random.split(jax.random.key(seed), 10)
    return {
        "queries": draw_queries(jax.random.fold_in(key_of[9], 71), 0),
        "positives": draw_positives(jax.random.fold_in(key_of[9], 71), 0),
        "label_vectors": draw_label_vectors(jax.random.fold_in(key_of[9], 71), 0),
        "refresh_slot": jax.random.randint(key_of[3], (), 0, SLOTS).astype(jnp.int32),
        "features": normal_values(key_of[4], (REFRESH, D), 1.0, 6.0, ((0, 256),)),
        "encoder_weight": normal_values(key_of[5], (D, D), D ** -0.5, 0.21875),
        "encoder_gain": jnp.clip(1.0 + 0.18 * jax.random.normal(key_of[6], (D,), jnp.float32), 0.1, 1.9),
        "free_vectors": normal_values(key_of[7], (REFRESH, D), 0.5, 3.0, ((0, 256),)),
        "targets": draw_targets(jax.random.fold_in(key_of[9], 71), 0),
    }


def reference(queries, positives, label_vectors, refresh_slot, features, encoder_weight, encoder_gain, free_vectors, targets):
    hidden = jnp.dot(features, encoder_weight, preferred_element_type=jnp.float32)
    normed = hidden * lax.rsqrt(lax.optimization_barrier(jnp.mean(hidden * hidden, axis=1, keepdims=True)) + 1e-06) * encoder_gain
    encoded = lax.optimization_barrier(normed.astype(jnp.bfloat16))
    placed = jnp.zeros((REFRESH, D), jnp.bfloat16).at[targets].set(encoded)
    refreshed = (free_vectors.astype(jnp.float32) + placed.astype(jnp.float32)).astype(jnp.bfloat16)
    blocks = label_vectors.reshape(N_CLS, SLOTS, R_DEV, D)
    zero_index = jnp.zeros((), jnp.int32)
    current = lax.dynamic_update_slice(blocks, refreshed.reshape(N_CLS, 1, R_DEV, D), (zero_index, refresh_slot.astype(jnp.int32), zero_index, zero_index)).reshape(LABELS, D)
    block_size = Q_DEV * 32
    query_blocks = queries.reshape(-1, block_size, D)
    positive_blocks = positives.reshape(-1, block_size, POS)

    def one_block(block_pair):
        block_queries, block_ids = block_pair
        logits = lax.dot_general(block_queries, current, (((1,), (1,)), ((), ())), preferred_element_type=jnp.float32)
        maximum = lax.optimization_barrier(jnp.max(logits, axis=1))
        exp_total = lax.optimization_barrier(jnp.sum(jnp.exp(logits - maximum[:, None]), axis=1))
        log_total = maximum + jnp.log(exp_total)
        valid_ids = block_ids >= 0
        safe_ids = jnp.where(valid_ids, block_ids, 0).astype(jnp.int32)
        picked = jnp.take_along_axis(logits, safe_ids, axis=1)
        id_count = lax.optimization_barrier(jnp.sum(valid_ids.astype(jnp.float32), axis=1))
        positive_sum = lax.optimization_barrier(jnp.sum(jnp.where(valid_ids, picked, jnp.zeros_like(picked)), axis=1))
        block_loss = log_total - positive_sum / id_count
        id_weight = jnp.where(valid_ids, jnp.ones_like(picked), jnp.zeros_like(picked)) / id_count[:, None]
        row_index = jnp.broadcast_to(jnp.arange(block_ids.shape[0], dtype=jnp.int32)[:, None], block_ids.shape)
        target_mass = jnp.zeros(logits.shape, jnp.float32).at[row_index, safe_ids].add(id_weight)
        coefficients = (jnp.exp(logits - log_total[:, None]) - target_mass).astype(jnp.bfloat16)
        block_grads = jnp.dot(coefficients, current, preferred_element_type=jnp.float32).astype(jnp.bfloat16)
        return (block_loss, block_grads)
    losses, grads = lax.map(one_block, (query_blocks, positive_blocks))
    return (losses.reshape(N_REP, QG), grads.reshape(N_REP, QG, D), refreshed)
```

```python
import functools

import jax
import jax.numpy as jnp
from jax import lax
from jax.experimental import pallas as pl
from jax.experimental.pallas import tpu as pltpu
from jax.sharding import Mesh
from jax.sharding import PartitionSpec as P

SLOTS = 8
D = 768
HALF = 384
QG = 256
N_CLS = 128
PER = 3
CLS = ("cls_0", "cls_1", "cls_2")
CLS_REP = ("cls_0", "cls_1", "cls_2", "rep")
SEND = PER * HALF + D
BACK = 2 * D + 128
F32 = jnp.float32
BF16 = jnp.bfloat16
VMEM = pltpu.VMEM
SMEM = pltpu.SMEM


def vmem_spec():
    return pl.BlockSpec(memory_space=VMEM)


def smem_spec():
    return pl.BlockSpec(memory_space=SMEM)


def iota(shape, dim):
    return lax.broadcasted_iota(jnp.int32, shape, dim)


def dot(a, b):
    return jnp.dot(a, b, preferred_element_type=F32)


def dot_last(a, b):
    return lax.dot_general(a, b, (((1,), (1,)), ((), ())), preferred_element_type=F32)


def dot_first(a, b):
    return lax.dot_general(a, b, (((0,), (0,)), ((), ())), preferred_element_type=F32)


def encode_kernel(idx_ref, feat_ref, weight_ref, gain_ref, tgt_ref, q_ref, out_ref):
    block = idx_ref[0]
    hidden = dot(feat_ref[...], weight_ref[...])
    mean = jnp.mean(hidden * hidden, axis=1, keepdims=True)
    encoded = (hidden * lax.rsqrt(mean + 1e-06) * gain_ref[...]).astype(BF16)
    rows = [tgt_ref[pl.ds(3 * block + a, 1), :].astype(F32) for a in range(3)]
    columns = [jnp.broadcast_to(row, (128, 128)).T for row in rows]
    ranks = []
    for row in rows:
        rank = jnp.zeros((1, 128), F32)
        for column in columns:
            rank += jnp.sum(jnp.where(column < row, 1.0, 0.0), axis=0, keepdims=True)
        ranks.append(rank)
    rank = jnp.concatenate(ranks, axis=1)
    line = iota((QG, HALF), 0)
    first = ((line >> 1) * PER).astype(F32)
    odd = (line & 1) == 1
    for k in range(PER):
        hit = rank == first + float(k)
        total = dot(jnp.where(hit & ~odd, 1.0, 0.0).astype(BF16), encoded[:, :HALF])
        total += dot(jnp.where(hit & odd, 1.0, 0.0).astype(BF16), encoded[:, HALF:])
        out_ref[:, k * HALF : (k + 1) * HALF] = total.astype(BF16)
    own = q_ref[...].astype(F32)
    wide_odd = (iota((QG, D), 0) & 1) == 1
    out_ref[:, PER * HALF :] = jnp.where(wide_odd, own[1:2], own[0:1]).astype(BF16)


def place_kernel(idx_ref, tgt_ref, out_ref):
    base = idx_ref[1] * (2 * HALF) + idx_ref[2] * HALF
    parts = [tgt_ref[pl.ds(3 * idx_ref[2] + a, N_CLS, stride=6), :] for a in range(3)]
    offsets = jnp.concatenate(parts, axis=1) - base
    inside = (offsets >= 0) & (offsets < HALF)
    far = 4096.0
    keys = jnp.where(inside, offsets.astype(F32), far)
    lane = iota((N_CLS, HALF), 1).astype(F32)
    source = iota((N_CLS, QG), 0)
    line = iota((N_CLS, QG), 1)
    spread = [
        jnp.where((line >> 1 == source) & ((line & 1) == h), 1.0, 0.0).astype(BF16)
        for h in range(2)
    ]
    for k in range(PER):
        least = jnp.min(keys, axis=1, keepdims=True)
        keys = jnp.where(keys == least, far, keys)
        chosen = jnp.where(lane == least, 1.0, 0.0).astype(BF16)
        for h in range(2):
            out_ref[2 * k + h] = dot_first(chosen, spread[h]).astype(BF16)


def refresh_kernel(place_ref, got_ref, free_ref, out_ref):
    for h in range(2):
        cols = slice(h * HALF, (h + 1) * HALF)
        placed = dot(place_ref[h], got_ref[:, :HALF])
        for k in range(1, PER):
            placed += dot(place_ref[2 * k + h], got_ref[:, k * HALF : (k + 1) * HALF])
        out_ref[:, cols] = (free_ref[:, cols].astype(F32) + placed).astype(BF16)


def count_hits(ids_ref, first, width):
    label = first + iota((QG, width), 1)
    hits = jnp.zeros((QG, width), F32)
    for k in range(4):
        hits += jnp.where(ids_ref[:, k : k + 1] == label, 1.0, 0.0)
    return hits.astype(BF16)


def positive_kernel(idx_ref, ids_ref, lab_ref, out_ref):
    step = pl.program_id(0)

    @pl.when(step == 0)
    def _():
        out_ref[...] = jnp.zeros_like(out_ref)

    slot = step + (step >= idx_ref[3]).astype(jnp.int32)
    first = idx_ref[1] * (SLOTS * D) + slot * D
    out_ref[...] += dot(count_hits(ids_ref, first, D), lab_ref[...])


def absorb(logits, vectors, m_prev, s_prev, acc_prev):
    m_new = m_prev
    for part in logits:
        m_new = jnp.maximum(m_new, jnp.max(part, axis=1, keepdims=True))
    scale = jnp.exp(m_prev - m_new)
    s_new = s_prev * scale
    acc_new = acc_prev * scale
    for part, rows in zip(logits, vectors):
        weight = jnp.exp(part - m_new)
        s_new += jnp.sum(weight, axis=1, keepdims=True)
        acc_new += dot(weight.astype(BF16), rows)
    return m_new, s_new, acc_new


def old_kernel(idx_ref, got_ref, lab_ref, m_ref, s_ref, acc_ref):
    step = pl.program_id(0)

    @pl.when(step == 0)
    def _():
        m_ref[...] = jnp.full_like(m_ref, -jnp.inf)
        s_ref[...] = jnp.zeros_like(s_ref)
        acc_ref[...] = jnp.zeros_like(acc_ref)

    logits = dot_last(got_ref[:, PER * HALF :], lab_ref[...])
    m_new, s_new, acc_new = absorb(
        [logits], [lab_ref[...]], m_ref[:, :1], s_ref[:, :1], acc_ref[...]
    )
    m_ref[...] = jnp.broadcast_to(m_new, m_ref.shape)
    s_ref[...] = jnp.broadcast_to(s_new, s_ref.shape)
    acc_ref[...] = acc_new


def three_parts(value):
    high = value.astype(BF16).astype(F32)
    rest = value - high
    middle = rest.astype(BF16).astype(F32)
    return [high, middle, rest - middle]


def fresh_kernel(idx_ref, ids_ref, got_ref, own_ref, other_ref, pos_ref, m_ref, s_ref, acc_ref, out_ref):
    queries = got_ref[:, PER * HALF :]
    vectors = [own_ref[...], other_ref[...]]
    logits = [dot_last(queries, rows) for rows in vectors]
    m_new, s_new, acc_new = absorb(logits, vectors, m_ref[:, :1], s_ref[:, :1], acc_ref[...])
    rep = idx_ref[2]
    first = idx_ref[1] * (SLOTS * D) + idx_ref[3] * D
    positive = pos_ref[...]
    for rows, half in zip(vectors, (rep, 1 - rep)):
        positive += dot(count_hits(ids_ref, first + half * HALF, HALF), rows)
    picked = jnp.sum(queries.astype(F32) * positive, axis=1, keepdims=True)
    lane = iota((QG, 128), 1)
    stats = jnp.zeros((QG, 128), F32)
    for at, part in enumerate(three_parts(m_new) + three_parts(s_new) + three_parts(picked)):
        stats = jnp.where(lane == at, part, stats)
    out_ref[:, :D] = acc_new.astype(BF16)
    out_ref[:, D : 2 * D] = positive.astype(BF16)
    out_ref[:, 2 * D :] = stats.astype(BF16)


def finish_kernel(inv_ref, back_ref, loss_ref, grad_ref):
    stats = back_ref[:, 2 * D :].astype(F32)

    def column(at):
        return stats[:, at : at + 1] + stats[:, at + 1 : at + 2] + stats[:, at + 2 : at + 3]

    peak, total, picked = column(0), column(3), column(6)
    odd = (iota((QG, 1), 0) & 1) == 1
    for h in range(2):
        mine = odd if h else ~odd
        top = jnp.max(jnp.where(mine, peak, -jnp.inf), axis=0, keepdims=True)
        weight = jnp.where(mine, jnp.exp(peak - top), 0.0)
        exp_total = jnp.sum(weight * total, axis=0, keepdims=True)
        inverse = inv_ref[h]
        chosen = jnp.sum(jnp.where(mine, picked, 0.0), axis=0, keepdims=True)
        loss = top + jnp.log(exp_total) - chosen * inverse
        loss_ref[h : h + 1, :] = jnp.broadcast_to(loss, (1, 128))
        scaled = back_ref[:, :D].astype(F32) * (weight / exp_total)
        scaled -= jnp.where(mine, back_ref[:, D : 2 * D].astype(F32), 0.0) * inverse
        grad_ref[h : h + 1, :] = jnp.sum(scaled, axis=0, keepdims=True)


def per_device(
    queries,
    positives,
    label_vectors,
    refresh_slot,
    features,
    encoder_weight,
    encoder_gain,
    free_vectors,
    targets,
):
    cls_index = lax.axis_index(CLS)
    rep_index = lax.axis_index("rep")
    idx = jnp.stack([cls_index * 2 + rep_index, cls_index, rep_index, refresh_slot]).astype(jnp.int32)
    target_rows = targets.reshape(768, 128)
    ids = lax.dynamic_index_in_dim(positives, rep_index, 0, keepdims=False)
    own_ids = lax.dynamic_slice_in_dim(ids, cls_index * 2, 2)
    inverse = 1.0 / jnp.sum((own_ids >= 0).astype(F32), axis=1)

    sending = pl.pallas_call(
        encode_kernel,
        out_shape=jax.ShapeDtypeStruct((QG, SEND), BF16),
        in_specs=[smem_spec()] + [vmem_spec()] * 5,
        out_specs=vmem_spec(),
        name="encode",
    )(idx, features, encoder_weight, encoder_gain.reshape(1, D), target_rows, queries.reshape(2, D))
    got = lax.all_to_all(sending.reshape(N_CLS, 2, SEND), CLS, 0, 0, tiled=True)
    got = got.reshape(QG, SEND)

    place = pl.pallas_call(
        place_kernel,
        out_shape=jax.ShapeDtypeStruct((2 * PER, HALF, QG), BF16),
        in_specs=[smem_spec(), vmem_spec()],
        out_specs=vmem_spec(),
        name="place",
    )(idx, target_rows)

    def slot_block(step, idx_ref):
        return (step + (step >= idx_ref[3]).astype(jnp.int32), 0)

    def whole(step, idx_ref):
        return (0, 0)

    slot_spec = pl.BlockSpec((D, D), slot_block)
    positive_old = pl.pallas_call(
        positive_kernel,
        out_shape=jax.ShapeDtypeStruct((QG, D), F32),
        grid_spec=pltpu.PrefetchScalarGridSpec(
            num_scalar_prefetch=1,
            grid=(SLOTS - 1,),
            in_specs=[pl.BlockSpec((QG, 4), whole), slot_spec],
            out_specs=pl.BlockSpec((QG, D), whole),
        ),
        name="positive",
    )(idx, ids, label_vectors)

    refreshed = pl.pallas_call(
        refresh_kernel,
        out_shape=jax.ShapeDtypeStruct((HALF, D), BF16),
        in_specs=[vmem_spec()] * 3,
        out_specs=vmem_spec(),
        name="refresh",
    )(place, got, free_vectors)
    partner = lax.ppermute(refreshed, "rep", [(0, 1), (1, 0)])

    state = pl.pallas_call(
        old_kernel,
        out_shape=[
            jax.ShapeDtypeStruct((QG, 128), F32),
            jax.ShapeDtypeStruct((QG, 128), F32),
            jax.ShapeDtypeStruct((QG, D), F32),
        ],
        grid_spec=pltpu.PrefetchScalarGridSpec(
            num_scalar_prefetch=1,
            grid=(SLOTS - 1,),
            in_specs=[pl.BlockSpec((QG, SEND), whole), slot_spec],
            out_specs=[
                pl.BlockSpec((QG, 128), whole),
                pl.BlockSpec((QG, 128), whole),
                pl.BlockSpec((QG, D), whole),
            ],
        ),
        name="old",
    )(idx, got, label_vectors)

    leaving = pl.pallas_call(
        fresh_kernel,
        out_shape=jax.ShapeDtypeStruct((QG, BACK), BF16),
        in_specs=[smem_spec()] + [vmem_spec()] * 8,
        out_specs=vmem_spec(),
        name="fresh",
    )(idx, ids, got, refreshed, partner, positive_old, *state)
    back = lax.all_to_all(leaving.reshape(N_CLS, 2, BACK), CLS, 0, 0, tiled=True)
    loss, grads = pl.pallas_call(
        finish_kernel,
        out_shape=[jax.ShapeDtypeStruct((2, 128), F32), jax.ShapeDtypeStruct((2, D), F32)],
        in_specs=[smem_spec(), vmem_spec()],
        out_specs=[vmem_spec()] * 2,
        name="finish",
    )(inverse, back.reshape(QG, BACK))
    return (
        loss[:, 0].reshape(1, 2),
        grads.astype(BF16).reshape(1, 2, D),
        refreshed,
    )


def solution(mesh):
    torus = Mesh(
        mesh.devices.reshape(4, 8, 4, mesh.shape["rep"]), ("cls_0", "cls_1", "cls_2", "rep")
    )
    placed = (
        P("rep", CLS, None),
        P(),
        P(CLS, None),
        P(),
        P(CLS_REP, None),
        P(),
        P(),
        P(CLS_REP, None),
        P(),
    )
    return jax.shard_map(
        per_device,
        mesh=torus,
        in_specs=placed,
        out_specs=(P("rep", CLS), P("rep", CLS, None), P(CLS_REP, None)),
        check_vma=False,
    )
```

```python
import jax
import jax.numpy as jnp
from jax import lax
from jax.experimental import pallas as pl
from jax.experimental.pallas import tpu as pltpu
from jax.sharding import Mesh
from jax.sharding import PartitionSpec as P

SLOTS = 8
OLD = SLOTS - 1
D = 768
HALF = 384
QG = 256
N_CLS = 128
PER = 3
CLS = ("cls_0", "cls_1", "cls_2")
CLS_REP = ("cls_0", "cls_1", "cls_2", "rep")
ROWS = PER * HALF
SEND = ROWS + D
BACK = 2 * D + 128
F32 = jnp.float32
BF16 = jnp.bfloat16


def vmem_spec():
    return pl.BlockSpec(memory_space=pltpu.VMEM)


def smem_spec():
    return pl.BlockSpec(memory_space=pltpu.SMEM)


def iota(shape, dim):
    return lax.broadcasted_iota(jnp.int32, shape, dim)


def dot(a, b):
    return jnp.dot(a, b, preferred_element_type=F32)


def dot_last(a, b):
    return lax.dot_general(a, b, (((1,), (1,)), ((), ())), preferred_element_type=F32)


def dot_first(a, b):
    return lax.dot_general(a, b, (((0,), (0,)), ((), ())), preferred_element_type=F32)


def one_hot(mask):
    return jnp.where(mask, 1.0, 0.0).astype(BF16)


def spread_down(row):
    return jnp.broadcast_to(row, (128, 128)).T


def encode_kernel(feat_ref, weight_ref, gain_ref, tgt_ref, q_ref, out_ref):
    block = lax.axis_index(CLS_REP)
    hidden = dot(feat_ref[...], weight_ref[...])
    mean = jnp.mean(hidden * hidden, axis=1, keepdims=True)
    gain = jnp.concatenate([gain_ref[i : i + 1, :] for i in range(6)], axis=1)
    encoded = (hidden * lax.rsqrt(mean + 1e-06) * gain).astype(BF16)
    rows = [tgt_ref[pl.ds(3 * block + a, 1), :].astype(F32) for a in range(3)]
    columns = [spread_down(row) for row in rows]
    ranks = []
    for row in rows:
        rank = jnp.zeros((1, 128), F32)
        for column in columns:
            rank += jnp.sum(jnp.where(column < row, 1.0, 0.0), axis=0, keepdims=True)
        ranks.append(rank)
    rank = jnp.concatenate(ranks, axis=1)
    line = iota((QG, HALF), 0)
    first = ((line >> 1) * PER).astype(F32)
    odd = (line & 1) == 1
    for k in range(PER):
        hit = rank == first + float(k)
        total = dot(one_hot(hit & ~odd), encoded[:, :HALF])
        total += dot(one_hot(hit & odd), encoded[:, HALF:])
        out_ref[..., k * HALF : (k + 1) * HALF] = total.astype(BF16).reshape(N_CLS, 2, HALF)
    out_ref[..., ROWS:] = jnp.broadcast_to(q_ref[...], (N_CLS, 2, D))


def place_kernel(tgt_ref, ids_ref, key_ref, plane_ref, flag_ref):
    cls_index, rep_index = lax.axis_index(CLS), lax.axis_index("rep")
    base = cls_index * (2 * HALF) + rep_index * HALF
    parts = [tgt_ref[pl.ds(3 * rep_index + a, N_CLS, stride=6), :] for a in range(3)]
    offsets = jnp.concatenate(parts, axis=1) - base
    inside = (offsets >= 0) & (offsets < HALF)
    far = 4096.0
    keys = jnp.where(inside, offsets.astype(F32), far)
    source = iota((N_CLS, QG), 0)
    twice = (iota((N_CLS, QG), 1) >> 1) == source
    for k in range(PER):
        least = jnp.min(keys, axis=1, keepdims=True)
        keys = jnp.where(keys == least, far, keys)
        wide = jnp.broadcast_to(least, (N_CLS, QG))
        key_ref[k : k + 1, :] = jnp.sum(jnp.where(twice, wide, 0.0), axis=0, keepdims=True)
    first = cls_index * (SLOTS * D)
    lane = iota((QG, 128), 1)
    seen = jnp.zeros((QG, 128), F32)
    for k in range(4):
        own = (ids_ref[rep_index, k : k + 1, :] - first).astype(F32)
        plane = jnp.concatenate([spread_down(own[:, :128]), spread_down(own[:, 128:])], axis=0)
        plane_ref[k] = plane
        seen = jnp.where((plane.astype(jnp.int32) >> 7) == lane, 1.0, seen)
    flag_ref[...] = jnp.max(seen, axis=0, keepdims=True).astype(jnp.int32)


def hits_of(plane_ref, first):
    label = iota((QG, 128), 1).astype(F32) + first.astype(F32)
    hits = jnp.zeros((QG, 128), F32)
    for k in range(4):
        hits += jnp.where(plane_ref[k] == label, 1.0, 0.0)
    return hits.astype(BF16)


def old_slot(step, slot_ref):
    return step + (step >= slot_ref[0]).astype(jnp.int32)


def positive_kernel(slot_ref, flag_ref, plane_ref, lab_ref, out_ref):
    step = pl.program_id(0)

    @pl.when(step == 0)
    def _():
        out_ref[...] = jnp.zeros_like(out_ref)

    slot = old_slot(step, slot_ref)
    for part in range(6):
        tile = slot * 6 + part

        @pl.when(flag_ref[0, tile] > 0)
        def _():
            rows = lab_ref[part * 128 : (part + 1) * 128, :]
            out_ref[...] += dot(hits_of(plane_ref, tile * 128), rows)


def refresh_kernel(key_ref, got_ref, free_ref, pos_ref, out_ref):
    own = iota((HALF, QG), 0).astype(F32)
    odd = (iota((HALF, QG), 1) & 1) == 1
    matches = [key_ref[k : k + 1, :] == own for k in range(PER)]
    got = [got_ref[..., k * HALF : (k + 1) * HALF].reshape(QG, HALF) for k in range(PER)]
    for h in range(2):
        cols = slice(h * HALF, (h + 1) * HALF)
        mine = odd if h else ~odd
        placed = jnp.zeros((HALF, HALF), F32)
        for k in range(PER):
            placed += dot(one_hot(matches[k] & mine), got[k])
        out_ref[:, cols] = (free_ref[:, cols].astype(F32) + placed).astype(BF16)


def three_parts(value):
    high = value.astype(BF16).astype(F32)
    rest = value - high
    middle = rest.astype(BF16).astype(F32)
    return [high, middle, rest - middle]


def over_lanes(fn, value):
    total = value[:, :128]
    for at in range(128, value.shape[1], 128):
        total = fn(total, value[:, at : at + 128])
    return total


def score_kernel(
    slot_ref, flag_ref, got_ref, own_ref, other_ref, lab_ref, plane_ref, pos_ref, out_ref,
    q_buf, lab_buf, plane_buf, pos_buf, sems,
):
    rep = lax.axis_index("rep")
    slot = slot_ref[0]

    def rows_at(first, size):
        return lab_buf.at[pl.ds(first, size), :]

    query_copy = pltpu.make_async_copy(got_ref.at[:, :, pl.ds(ROWS, D)], q_buf, sems.at[SLOTS])
    query_copy.start()
    lab_copies = []
    for i in range(OLD):
        source = (i + (i >= slot).astype(jnp.int32)) * D
        lab_copies.append(
            pltpu.make_async_copy(lab_ref.at[pl.ds(source, D), :], rows_at(i * D, D), sems.at[i])
        )
        lab_copies[-1].start()
    own_copy = pltpu.make_async_copy(
        own_ref, rows_at(OLD * D + rep * HALF, HALF), sems.at[OLD]
    )
    other_copy = pltpu.make_async_copy(
        other_ref, rows_at(OLD * D + (1 - rep) * HALF, HALF), sems.at[SLOTS + 1]
    )
    plane_copy = pltpu.make_async_copy(plane_ref, plane_buf, sems.at[SLOTS + 2])
    pos_copy = pltpu.make_async_copy(pos_ref, pos_buf, sems.at[SLOTS + 3])
    for copy in (own_copy, other_copy, plane_copy, pos_copy):
        copy.start()
    query_copy.wait()
    queries = q_buf[...].reshape(QG, D)

    def logits_of(i):
        if i < OLD:
            lab_copies[i].wait()
        else:
            own_copy.wait()
            other_copy.wait()
        return dot_last(queries, lab_buf[i * D : (i + 1) * D, :])

    peak = jnp.full((QG, 1), -jnp.inf, F32)
    total = jnp.zeros((QG, 128), F32)
    grads = jnp.zeros((QG, D), F32)
    following = logits_of(0)
    for i in range(SLOTS):
        logits = following
        if i + 1 < SLOTS:
            following = logits_of(i + 1)
        higher = jnp.maximum(peak, jnp.max(over_lanes(jnp.maximum, logits), axis=1, keepdims=True))
        scale = jnp.exp(peak - higher)
        weight = jnp.exp(logits - higher)
        total = total * scale + over_lanes(jnp.add, weight)
        grads = grads * scale + dot(weight.astype(BF16), lab_buf[i * D : (i + 1) * D, :])
        peak = higher
    out_ref[..., :D] = grads.astype(BF16).reshape(N_CLS, 2, D)
    plane_copy.wait()
    pos_copy.wait()
    for part in range(6):
        tile = slot * 6 + part

        @pl.when(flag_ref[0, tile] > 0)
        def _():
            rows = lab_buf[OLD * D + part * 128 : OLD * D + (part + 1) * 128, :]
            pos_buf[...] += dot(hits_of(plane_buf, tile * 128), rows)

    positive = pos_buf[...]
    out_ref[..., D : 2 * D] = positive.astype(BF16).reshape(N_CLS, 2, D)
    picked = jnp.sum(queries.astype(F32) * positive, axis=1, keepdims=True)
    exp_total = jnp.sum(total, axis=1, keepdims=True)
    lane = iota((QG, 128), 1)
    stats = jnp.zeros((QG, 128), F32)
    for at, part in enumerate(three_parts(peak) + three_parts(exp_total) + three_parts(picked)):
        stats = jnp.where(lane == at, part, stats)
    out_ref[..., 2 * D :] = stats.astype(BF16).reshape(N_CLS, 2, 128)


def finish_kernel(ids_ref, back_ref, loss_ref, grad_ref):
    back = back_ref[...].reshape(QG, BACK)
    stats = back[:, 2 * D :].astype(F32)

    def column(at):
        return stats[:, at : at + 1] + stats[:, at + 1 : at + 2] + stats[:, at + 2 : at + 3]

    peak, total, picked = column(0), column(3), column(6)
    odd = (iota((QG, 1), 0) & 1) == 1
    valid = jnp.where(ids_ref[lax.axis_index("rep")] >= 0, 1.0, 0.0)
    column_of = iota((4, QG), 1) - 2 * lax.axis_index(CLS)
    losses, grads = [], []
    for h in range(2):
        mine = odd if h else ~odd
        top = jnp.max(jnp.where(mine, peak, -jnp.inf), axis=0, keepdims=True)
        weight = jnp.where(mine, jnp.exp(peak - top), 0.0)
        exp_total = jnp.sum(weight * total, axis=0, keepdims=True)
        count = jnp.sum(jnp.where(column_of == h, valid, 0.0), axis=1, keepdims=True)
        inverse = 1.0 / jnp.sum(count, axis=0, keepdims=True)
        chosen = jnp.sum(jnp.where(mine, picked, 0.0), axis=0, keepdims=True)
        losses.append(top + jnp.log(exp_total) - chosen * inverse)
        scaled = back[:, :D].astype(F32) * (weight / exp_total)
        scaled -= jnp.where(mine, back[:, D : 2 * D].astype(F32), 0.0) * inverse
        grads.append(jnp.sum(scaled, axis=0, keepdims=True))
    loss_ref[...] = jnp.concatenate(losses, axis=1)
    grad_ref[...] = jnp.concatenate(grads, axis=0).astype(BF16).reshape(1, 2, D)


def per_device(
    queries,
    positives,
    label_vectors,
    refresh_slot,
    features,
    encoder_weight,
    encoder_gain,
    free_vectors,
    targets,
):
    target_rows = targets.reshape(768, 128)
    slot = refresh_slot.reshape(1)
    ids = positives.transpose(0, 2, 1)

    sending = pl.pallas_call(
        encode_kernel,
        out_shape=jax.ShapeDtypeStruct((N_CLS, 2, SEND), BF16),
        in_specs=[vmem_spec()] * 5,
        out_specs=vmem_spec(),
        name="encode",
    )(features, encoder_weight, encoder_gain.reshape(6, 128), target_rows, queries)
    keys, planes, flags = pl.pallas_call(
        place_kernel,
        out_shape=[
            jax.ShapeDtypeStruct((8, QG), F32),
            jax.ShapeDtypeStruct((4, QG, 128), F32),
            jax.ShapeDtypeStruct((1, 128), jnp.int32),
        ],
        in_specs=[vmem_spec()] * 2,
        out_specs=[vmem_spec()] * 3,
        name="place",
    )(target_rows, ids)
    got = lax.all_to_all(sending, CLS, 0, 0, tiled=True)

    def all_of(shape):
        return pl.BlockSpec(shape, lambda *args: (0,) * len(shape))

    positive_old = pl.pallas_call(
        positive_kernel,
        out_shape=jax.ShapeDtypeStruct((QG, D), F32),
        grid_spec=pltpu.PrefetchScalarGridSpec(
            num_scalar_prefetch=2,
            grid=(OLD,),
            in_specs=[
                all_of((4, QG, 128)),
                pl.BlockSpec((D, D), lambda step, slot_ref, flag_ref: (old_slot(step, slot_ref), 0)),
            ],
            out_specs=all_of((QG, D)),
        ),
        name="positive",
    )(slot, flags, planes, label_vectors)

    refreshed = pl.pallas_call(
        refresh_kernel,
        out_shape=jax.ShapeDtypeStruct((HALF, D), BF16),
        grid=(1,),
        in_specs=[
            all_of((8, QG)),
            pl.BlockSpec((N_CLS, 2, ROWS), lambda step: (0, 0, 0)),
            all_of((HALF, D)),
            pl.BlockSpec(memory_space=pl.ANY),
        ],
        out_specs=all_of((HALF, D)),
        name="refresh",
    )(keys, got, free_vectors, positive_old)
    partner = lax.ppermute(refreshed, "rep", [(0, 1), (1, 0)])

    any_spec = pl.BlockSpec(memory_space=pl.ANY)
    leaving = pl.pallas_call(
        score_kernel,
        out_shape=jax.ShapeDtypeStruct((N_CLS, 2, BACK), BF16),
        in_specs=[smem_spec(), smem_spec()] + [any_spec] * 6,
        out_specs=vmem_spec(),
        scratch_shapes=[
            pltpu.VMEM((N_CLS, 2, D), BF16),
            pltpu.VMEM((SLOTS * D, D), BF16),
            pltpu.VMEM((4, QG, 128), F32),
            pltpu.VMEM((QG, D), F32),
            pltpu.SemaphoreType.DMA((SLOTS + 4,)),
        ],
        name="score",
    )(slot, flags, got, refreshed, partner, label_vectors, planes, positive_old)
    back = lax.all_to_all(leaving, CLS, 0, 0, tiled=True)
    loss, grads = pl.pallas_call(
        finish_kernel,
        out_shape=[jax.ShapeDtypeStruct((1, 2), F32), jax.ShapeDtypeStruct((1, 2, D), BF16)],
        in_specs=[vmem_spec()] * 2,
        out_specs=[vmem_spec()] * 2,
        name="finish",
    )(ids, back)
    return loss, grads, refreshed


def solution(mesh):
    torus = Mesh(
        mesh.devices.reshape(4, 8, 4, mesh.shape["rep"]), ("cls_0", "cls_1", "cls_2", "rep")
    )
    placed = (
        P("rep", CLS, None),
        P(),
        P(CLS, None),
        P(),
        P(CLS_REP, None),
        P(),
        P(),
        P(CLS_REP, None),
        P(),
    )
    return jax.shard_map(
        per_device,
        mesh=torus,
        in_specs=placed,
        out_specs=(P("rep", CLS), P("rep", CLS, None), P(CLS_REP, None)),
        check_vma=False,
    )
```

```python
import jax
import jax.numpy as jnp
from jax import lax
from jax.experimental import pallas as pl
from jax.experimental.pallas import tpu as pltpu
from jax.sharding import Mesh
from jax.sharding import PartitionSpec as P

SLOTS = 8
OLD = SLOTS - 1
D = 768
HALF = 384
QG = 256
N_CLS = 128
PER = 3
CLS = ("cls_0", "cls_1", "cls_2")
CLS_REP = ("cls_0", "cls_1", "cls_2", "rep")
ROWS = PER * HALF
BACK = 2 * D + 128
F32 = jnp.float32
BF16 = jnp.bfloat16


def vmem_spec():
    return pl.BlockSpec(memory_space=pltpu.VMEM)


def smem_spec():
    return pl.BlockSpec(memory_space=pltpu.SMEM)


def iota(shape, dim):
    return lax.broadcasted_iota(jnp.int32, shape, dim)


def dot(a, b):
    return jnp.dot(a, b, preferred_element_type=F32)


def dot_last(a, b):
    return lax.dot_general(a, b, (((1,), (1,)), ((), ())), preferred_element_type=F32)


def dot_first(a, b):
    return lax.dot_general(a, b, (((0,), (0,)), ((), ())), preferred_element_type=F32)


def one_hot(mask):
    return jnp.where(mask, 1.0, 0.0).astype(BF16)


def spread_down(row):
    return jnp.broadcast_to(row, (128, 128)).T


def encode_kernel(feat_ref, weight_ref, gain_ref, tgt_ref, out_ref):
    block = lax.axis_index(CLS_REP)
    hidden = dot(feat_ref[...], weight_ref[...])
    mean = jnp.mean(hidden * hidden, axis=1, keepdims=True)
    gain = jnp.concatenate([gain_ref[i : i + 1, :] for i in range(6)], axis=1)
    encoded = (hidden * lax.rsqrt(mean + 1e-06) * gain).astype(BF16)
    rows = [tgt_ref[pl.ds(3 * block + a, 1), :].astype(F32) for a in range(3)]
    columns = [spread_down(row) for row in rows]
    ranks = []
    for row in rows:
        rank = jnp.zeros((1, 128), F32)
        for column in columns:
            rank += jnp.sum(jnp.where(column < row, 1.0, 0.0), axis=0, keepdims=True)
        ranks.append(rank)
    rank = jnp.concatenate(ranks, axis=1)
    line = iota((QG, HALF), 0)
    first = ((line >> 1) * PER).astype(F32)
    odd = (line & 1) == 1
    for k in range(PER):
        hit = rank == first + float(k)
        total = dot(one_hot(hit & ~odd), encoded[:, :HALF])
        total += dot(one_hot(hit & odd), encoded[:, HALF:])
        out_ref[..., k * HALF : (k + 1) * HALF] = total.astype(BF16).reshape(N_CLS, 2, HALF)


def place_kernel(tgt_ref, ids_ref, key_ref, plane_ref, flag_ref):
    cls_index, rep_index = lax.axis_index(CLS), lax.axis_index("rep")
    base = cls_index * (2 * HALF) + rep_index * HALF
    parts = [tgt_ref[pl.ds(3 * rep_index + a, N_CLS, stride=6), :] for a in range(3)]
    offsets = jnp.concatenate(parts, axis=1) - base
    inside = (offsets >= 0) & (offsets < HALF)
    far = 4096.0
    keys = jnp.where(inside, offsets.astype(F32), far)
    source = iota((N_CLS, QG), 0)
    twice = (iota((N_CLS, QG), 1) >> 1) == source
    for k in range(PER):
        least = jnp.min(keys, axis=1, keepdims=True)
        keys = jnp.where(keys == least, far, keys)
        wide = jnp.broadcast_to(least, (N_CLS, QG))
        key_ref[k : k + 1, :] = jnp.sum(jnp.where(twice, wide, 0.0), axis=0, keepdims=True)
    first = cls_index * (SLOTS * D)
    lane = iota((QG, 128), 1)
    seen = jnp.zeros((QG, 128), F32)
    for k in range(4):
        own = (ids_ref[rep_index, k : k + 1, :] - first).astype(F32)
        plane = jnp.concatenate([spread_down(own[:, :128]), spread_down(own[:, 128:])], axis=0)
        plane_ref[k] = plane
        seen = jnp.where((plane.astype(jnp.int32) >> 7) == lane, 1.0, seen)
    flag_ref[...] = jnp.max(seen, axis=0, keepdims=True).astype(jnp.int32)


def hits_of(plane_ref, first):
    label = iota((QG, 128), 1).astype(F32) + first.astype(F32)
    hits = jnp.zeros((QG, 128), F32)
    for k in range(4):
        hits += jnp.where(plane_ref[k] == label, 1.0, 0.0)
    return hits.astype(BF16)


def positive_kernel(slot_ref, flag_ref, plane_ref, lab_ref, out_ref, lab_buf, sems):
    out_ref[...] = jnp.zeros_like(out_ref)

    def copy_of(i, part):
        tile = (i + (i >= slot_ref[0]).astype(jnp.int32)) * 6 + part
        at = i * 6 + part
        return tile, pltpu.make_async_copy(
            lab_ref.at[pl.ds(tile * 128, 128), :], lab_buf.at[at], sems.at[at]
        )

    for i in range(OLD):
        for part in range(6):
            tile, copy = copy_of(i, part)
            pl.when(flag_ref[0, tile] > 0)(copy.start)

    def body(at, carry):
        i = at // 6
        tile, copy = copy_of(i, at - i * 6)

        @pl.when(flag_ref[0, tile] > 0)
        def _():
            copy.wait()
            out_ref[...] += dot(hits_of(plane_ref, tile * 128), lab_buf[at])

        return carry

    lax.fori_loop(0, OLD * 6, body, 0)


def refresh_kernel(key_ref, got_ref, free_ref, pos_ref, peak_ref, out_ref):
    own = iota((HALF, QG), 0).astype(F32)
    odd = (iota((HALF, QG), 1) & 1) == 1
    matches = [key_ref[k : k + 1, :] == own for k in range(PER)]
    got = [got_ref[..., k * HALF : (k + 1) * HALF].reshape(QG, HALF) for k in range(PER)]
    for h in range(2):
        cols = slice(h * HALF, (h + 1) * HALF)
        mine = odd if h else ~odd
        placed = jnp.zeros((HALF, HALF), F32)
        for k in range(PER):
            placed += dot(one_hot(matches[k] & mine), got[k])
        out_ref[:, cols] = (free_ref[:, cols].astype(F32) + placed).astype(BF16)


def over_lanes(fn, value):
    total = value[:, :128]
    for at in range(128, value.shape[1], 128):
        total = fn(total, value[:, at : at + 128])
    return total


def absorb(state, logits, rows):
    peak, total, grads = state
    higher = jnp.maximum(peak, jnp.max(over_lanes(jnp.maximum, logits), axis=1, keepdims=True))
    scale = jnp.exp(peak - higher)
    weight = jnp.exp(logits - higher)
    total = total * scale + over_lanes(jnp.add, weight)
    grads = grads * scale + dot(weight.astype(BF16), rows)
    return higher, total, grads


def old_kernel(slot_ref, *refs):
    pieces, (lab_ref, q_ref, peak_ref, total_ref, grad_ref, lab_buf, sems) = refs[:4], refs[4:]
    copies = []
    for i in range(OLD):
        source = (i + (i >= slot_ref[0]).astype(jnp.int32)) * D
        copies.append(
            pltpu.make_async_copy(lab_ref.at[pl.ds(source, D), :], lab_buf.at[i], sems.at[i])
        )
        copies[-1].start()
    line, lane = iota((QG, 64), 0), iota((QG, 64), 1)
    behind_y = (lax.axis_index("cls_0") - (line >> 6)) & 3
    behind_x = (lax.axis_index("cls_2") - ((line >> 1) & 3)) & 3
    spot = behind_x * 16 + ((line >> 3) & 7) * 2 + (line & 1)
    ordered = jnp.zeros((QG, D), F32)
    for back, piece_ref in enumerate(pieces):
        ordered += dot(one_hot((spot == lane) & (behind_y == back)), piece_ref[...])
    queries = ordered.astype(BF16)
    q_ref[...] = queries

    def logits_of(i):
        copies[i].wait()
        return dot_last(queries, lab_buf[i])

    state = (jnp.full((QG, 1), -jnp.inf, F32), jnp.zeros((QG, 128), F32), jnp.zeros((QG, D), F32))
    following = logits_of(0)
    for i in range(OLD):
        logits = following
        if i + 1 < OLD:
            following = logits_of(i + 1)
        state = absorb(state, logits, lab_buf[i])
    peak_ref[...] = jnp.broadcast_to(state[0], (QG, 128))
    total_ref[...] = state[1]
    grad_ref[...] = state[2]


def three_parts(value):
    high = value.astype(BF16).astype(F32)
    rest = value - high
    middle = rest.astype(BF16).astype(F32)
    return [high, middle, rest - middle]


def fresh_kernel(
    slot_ref, flag_ref, own_ref, other_ref, q_ref, peak_ref, total_ref, grad_ref, plane_ref,
    pos_ref, out_ref, own_buf, other_buf, q_buf, peak_buf, total_buf, grad_buf, plane_buf,
    pos_buf, sems,
):
    rep = lax.axis_index("rep")
    slot = slot_ref[0]
    pairs = [
        (q_ref, q_buf), (own_ref, own_buf), (other_ref, other_buf), (peak_ref, peak_buf),
        (total_ref, total_buf), (grad_ref, grad_buf), (plane_ref, plane_buf), (pos_ref, pos_buf),
    ]
    copies = [pltpu.make_async_copy(a, b, sems.at[i]) for i, (a, b) in enumerate(pairs)]
    for copy in copies:
        copy.start()
    copies[0].wait()
    copies[1].wait()
    queries = q_buf[...]
    own_logits = dot_last(queries, own_buf[...])
    copies[2].wait()
    other_logits = dot_last(queries, other_buf[...])
    for copy in copies[3:]:
        copy.wait()
    rows = jnp.concatenate([own_buf[...], other_buf[...]], axis=0)
    state = (peak_buf[:, :1], total_buf[...], grad_buf[...])
    peak, total, grads = absorb(state, jnp.concatenate([own_logits, other_logits], axis=1), rows)
    out_ref[..., :D] = grads.astype(BF16).reshape(N_CLS, 2, D)
    for buf, half in ((own_buf, rep), (other_buf, 1 - rep)):
        for part in range(3):
            tile = slot * 6 + half * 3 + part

            @pl.when(flag_ref[0, tile] > 0)
            def _():
                chosen = buf[part * 128 : (part + 1) * 128, :]
                pos_buf[...] += dot(hits_of(plane_buf, tile * 128), chosen)

    positive = pos_buf[...]
    out_ref[..., D : 2 * D] = positive.astype(BF16).reshape(N_CLS, 2, D)
    picked = jnp.sum(queries.astype(F32) * positive, axis=1, keepdims=True)
    exp_total = jnp.sum(total, axis=1, keepdims=True)
    lane = iota((QG, 128), 1)
    stats = jnp.zeros((QG, 128), F32)
    for at, part in enumerate(three_parts(peak) + three_parts(exp_total) + three_parts(picked)):
        stats = jnp.where(lane == at, part, stats)
    out_ref[..., 2 * D :] = stats.astype(BF16).reshape(N_CLS, 2, 128)


def finish_kernel(ids_ref, back_ref, loss_ref, grad_ref):
    back = back_ref[...].reshape(QG, BACK)
    stats = back[:, 2 * D :].astype(F32)

    def column(at):
        return stats[:, at : at + 1] + stats[:, at + 1 : at + 2] + stats[:, at + 2 : at + 3]

    peak, total, picked = column(0), column(3), column(6)
    odd = (iota((QG, 1), 0) & 1) == 1
    valid = jnp.where(ids_ref[lax.axis_index("rep")] >= 0, 1.0, 0.0)
    column_of = iota((4, QG), 1) - 2 * lax.axis_index(CLS)
    losses, grads = [], []
    for h in range(2):
        mine = odd if h else ~odd
        top = jnp.max(jnp.where(mine, peak, -jnp.inf), axis=0, keepdims=True)
        weight = jnp.where(mine, jnp.exp(peak - top), 0.0)
        exp_total = jnp.sum(weight * total, axis=0, keepdims=True)
        count = jnp.sum(jnp.where(column_of == h, valid, 0.0), axis=1, keepdims=True)
        inverse = 1.0 / jnp.sum(count, axis=0, keepdims=True)
        chosen = jnp.sum(jnp.where(mine, picked, 0.0), axis=0, keepdims=True)
        losses.append(top + jnp.log(exp_total) - chosen * inverse)
        scaled = back[:, :D].astype(F32) * (weight / exp_total)
        scaled -= jnp.where(mine, back[:, D : 2 * D].astype(F32), 0.0) * inverse
        grads.append(jnp.sum(scaled, axis=0, keepdims=True))
    loss_ref[...] = jnp.concatenate(losses, axis=1)
    grad_ref[...] = jnp.concatenate(grads, axis=0).astype(BF16).reshape(1, 2, D)


def from_behind(value, axis, shift):
    length = lax.axis_size(axis)
    return lax.ppermute(value, axis, [(i, (i + shift) % length) for i in range(length)])


def per_device(
    queries,
    positives,
    label_vectors,
    refresh_slot,
    features,
    encoder_weight,
    encoder_gain,
    free_vectors,
    targets,
):
    target_rows = targets.reshape(768, 128)
    slot = refresh_slot.reshape(1)
    ids = positives.transpose(0, 2, 1)

    column = lax.all_to_all(
        jnp.broadcast_to(queries.reshape(1, 2, D), (8, 2, D)), "cls_1", 0, 0, tiled=True
    )
    sending = pl.pallas_call(
        encode_kernel,
        out_shape=jax.ShapeDtypeStruct((N_CLS, 2, ROWS), BF16),
        in_specs=[vmem_spec()] * 4,
        out_specs=vmem_spec(),
        name="encode",
    )(features, encoder_weight, encoder_gain.reshape(6, 128), target_rows)
    keys, planes, flags = pl.pallas_call(
        place_kernel,
        out_shape=[
            jax.ShapeDtypeStruct((8, QG), F32),
            jax.ShapeDtypeStruct((4, QG, 128), F32),
            jax.ShapeDtypeStruct((1, 128), jnp.int32),
        ],
        in_specs=[vmem_spec()] * 2,
        out_specs=[vmem_spec()] * 3,
        name="place",
    )(target_rows, ids)
    sending, column = lax.optimization_barrier((sending, column))
    got = lax.all_to_all(sending, CLS, 0, 0, tiled=True)

    column = column.reshape(16, D)
    row = [column] + [from_behind(column, "cls_2", shift) for shift in (1, 2, 3)]
    layer = jnp.concatenate(row, axis=0)
    pieces = [layer] + [from_behind(layer, "cls_0", shift) for shift in (1, 2, 3)]

    any_spec = pl.BlockSpec(memory_space=pl.ANY)
    positive_old = pl.pallas_call(
        positive_kernel,
        out_shape=jax.ShapeDtypeStruct((QG, D), F32),
        in_specs=[smem_spec()] * 2 + [vmem_spec(), any_spec],
        out_specs=vmem_spec(),
        scratch_shapes=[
            pltpu.VMEM((OLD * 6, 128, D), BF16),
            pltpu.SemaphoreType.DMA((OLD * 6,)),
        ],
        name="positive",
    )(slot, flags, planes, label_vectors)

    all_queries, peak, total, grads = pl.pallas_call(
        old_kernel,
        out_shape=[
            jax.ShapeDtypeStruct((QG, D), BF16),
            jax.ShapeDtypeStruct((QG, 128), F32),
            jax.ShapeDtypeStruct((QG, 128), F32),
            jax.ShapeDtypeStruct((QG, D), F32),
        ],
        in_specs=[smem_spec()] + [vmem_spec()] * 4 + [any_spec],
        out_specs=[vmem_spec()] * 4,
        scratch_shapes=[pltpu.VMEM((OLD, D, D), BF16), pltpu.SemaphoreType.DMA((OLD,))],
        name="old",
    )(slot, *pieces, label_vectors)

    refreshed = pl.pallas_call(
        refresh_kernel,
        out_shape=jax.ShapeDtypeStruct((HALF, D), BF16),
        in_specs=[vmem_spec()] * 3 + [any_spec] * 2,
        out_specs=vmem_spec(),
        name="refresh",
    )(keys, got, free_vectors, positive_old, peak)
    partner = lax.ppermute(refreshed, "rep", [(0, 1), (1, 0)])

    leaving = pl.pallas_call(
        fresh_kernel,
        out_shape=jax.ShapeDtypeStruct((N_CLS, 2, BACK), BF16),
        in_specs=[smem_spec()] * 2 + [any_spec] * 8,
        out_specs=vmem_spec(),
        scratch_shapes=[
            pltpu.VMEM((HALF, D), BF16),
            pltpu.VMEM((HALF, D), BF16),
            pltpu.VMEM((QG, D), BF16),
            pltpu.VMEM((QG, 128), F32),
            pltpu.VMEM((QG, 128), F32),
            pltpu.VMEM((QG, D), F32),
            pltpu.VMEM((4, QG, 128), F32),
            pltpu.VMEM((QG, D), F32),
            pltpu.SemaphoreType.DMA((8,)),
        ],
        name="fresh",
    )(slot, flags, refreshed, partner, all_queries, peak, total, grads, planes, positive_old)
    back = lax.all_to_all(leaving, CLS, 0, 0, tiled=True)
    loss, grads = pl.pallas_call(
        finish_kernel,
        out_shape=[jax.ShapeDtypeStruct((1, 2), F32), jax.ShapeDtypeStruct((1, 2, D), BF16)],
        in_specs=[vmem_spec()] * 2,
        out_specs=[vmem_spec()] * 2,
        name="finish",
    )(ids, back)
    return loss, grads, refreshed


def solution(mesh):
    torus = Mesh(
        mesh.devices.reshape(4, 8, 4, mesh.shape["rep"]), ("cls_0", "cls_1", "cls_2", "rep")
    )
    placed = (
        P("rep", CLS, None),
        P(),
        P(CLS, None),
        P(),
        P(CLS_REP, None),
        P(),
        P(),
        P(CLS_REP, None),
        P(),
    )
    return jax.shard_map(
        per_device,
        mesh=torus,
        in_specs=placed,
        out_specs=(P("rep", CLS), P("rep", CLS, None), P(CLS_REP, None)),
        check_vma=False,
    )
```

```python
import jax
import jax.numpy as jnp
from jax import lax
from jax.experimental import pallas as pl
from jax.experimental.pallas import tpu as pltpu
from jax.sharding import Mesh
from jax.sharding import PartitionSpec as P

SLOTS = 8
OLD = SLOTS - 1
D = 768
HALF = 384
QG = 256
N_CLS = 128
PER = 3
CLS = ("cls_0", "cls_1", "cls_2")
CLS_REP = ("cls_0", "cls_1", "cls_2", "rep")
ROWS = PER * HALF
SEND = ROWS + D
BACK = 2 * D + 128
F32 = jnp.float32
BF16 = jnp.bfloat16
PARAMS = pltpu.CompilerParams(vmem_limit_bytes=24 * 1024 * 1024)


def vmem_spec():
    return pl.BlockSpec(memory_space=pltpu.VMEM)


def smem_spec():
    return pl.BlockSpec(memory_space=pltpu.SMEM)


def iota(shape, dim):
    return lax.broadcasted_iota(jnp.int32, shape, dim)


def dot(a, b):
    return jnp.dot(a, b, preferred_element_type=F32)


def dot_last(a, b):
    return lax.dot_general(a, b, (((1,), (1,)), ((), ())), preferred_element_type=F32)


def dot_first(a, b):
    return lax.dot_general(a, b, (((0,), (0,)), ((), ())), preferred_element_type=F32)


def one_hot(mask):
    return jnp.where(mask, 1.0, 0.0).astype(BF16)


def spread_down(row):
    return jnp.broadcast_to(row, (128, 128)).T


def encode_kernel(feat_ref, weight_ref, gain_ref, tgt_ref, q_ref, out_ref):
    block = lax.axis_index(CLS_REP)
    hidden = dot(feat_ref[...], weight_ref[...])
    mean = jnp.mean(hidden * hidden, axis=1, keepdims=True)
    gain = jnp.concatenate([gain_ref[i : i + 1, :] for i in range(6)], axis=1)
    encoded = (hidden * lax.rsqrt(mean + 1e-06) * gain).astype(BF16)
    rows = [tgt_ref[pl.ds(3 * block + a, 1), :].astype(F32) for a in range(3)]
    columns = [spread_down(row) for row in rows]
    ranks = []
    for row in rows:
        rank = jnp.zeros((1, 128), F32)
        for column in columns:
            rank += jnp.sum(jnp.where(column < row, 1.0, 0.0), axis=0, keepdims=True)
        ranks.append(rank)
    rank = jnp.concatenate(ranks, axis=1)
    line = iota((QG, HALF), 0)
    first = ((line >> 1) * PER).astype(F32)
    odd = (line & 1) == 1
    for k in range(PER):
        hit = rank == first + float(k)
        total = dot(one_hot(hit & ~odd), encoded[:, :HALF])
        total += dot(one_hot(hit & odd), encoded[:, HALF:])
        out_ref[..., k * HALF : (k + 1) * HALF] = total.astype(BF16).reshape(N_CLS, 2, HALF)
    out_ref[..., ROWS:] = jnp.broadcast_to(q_ref[...], (N_CLS, 2, D))


def place_kernel(tgt_ref, ids_ref, key_ref, plane_ref, flag_ref):
    cls_index, rep_index = lax.axis_index(CLS), lax.axis_index("rep")
    base = cls_index * (2 * HALF) + rep_index * HALF
    parts = [tgt_ref[pl.ds(3 * rep_index + a, N_CLS, stride=6), :] for a in range(3)]
    offsets = jnp.concatenate(parts, axis=1) - base
    inside = (offsets >= 0) & (offsets < HALF)
    far = 4096.0
    keys = jnp.where(inside, offsets.astype(F32), far)
    source = iota((N_CLS, QG), 0)
    twice = (iota((N_CLS, QG), 1) >> 1) == source
    for k in range(PER):
        least = jnp.min(keys, axis=1, keepdims=True)
        keys = jnp.where(keys == least, far, keys)
        wide = jnp.broadcast_to(least, (N_CLS, QG))
        key_ref[k : k + 1, :] = jnp.sum(jnp.where(twice, wide, 0.0), axis=0, keepdims=True)
    first = cls_index * (SLOTS * D)
    lane = iota((QG, 128), 1)
    seen = jnp.zeros((QG, 128), F32)
    for k in range(4):
        own = (ids_ref[rep_index, k : k + 1, :] - first).astype(F32)
        plane = jnp.concatenate([spread_down(own[:, :128]), spread_down(own[:, 128:])], axis=0)
        plane_ref[k] = plane
        seen = jnp.where((plane.astype(jnp.int32) >> 7) == lane, 1.0, seen)
    flag_ref[...] = jnp.max(seen, axis=0, keepdims=True).astype(jnp.int32)


def hits_of(plane_ref, first):
    label = iota((QG, 128), 1).astype(F32) + first.astype(F32)
    hits = jnp.zeros((QG, 128), F32)
    for k in range(4):
        hits += jnp.where(plane_ref[k] == label, 1.0, 0.0)
    return hits.astype(BF16)


def positive_kernel(slot_ref, flag_ref, plane_ref, lab_ref, out_ref, lab_buf, sems):
    out_ref[...] = jnp.zeros_like(out_ref)

    def copy_of(i, part):
        tile = (i + (i >= slot_ref[0]).astype(jnp.int32)) * 6 + part
        at = i * 6 + part
        return tile, pltpu.make_async_copy(
            lab_ref.at[pl.ds(tile * 128, 128), :], lab_buf.at[at], sems.at[at]
        )

    for i in range(OLD):
        for part in range(6):
            tile, copy = copy_of(i, part)
            pl.when(flag_ref[0, tile] > 0)(copy.start)

    def body(at, carry):
        i = at // 6
        tile, copy = copy_of(i, at - i * 6)

        @pl.when(flag_ref[0, tile] > 0)
        def _():
            copy.wait()
            out_ref[...] += dot(hits_of(plane_ref, tile * 128), lab_buf[at])

        return carry

    lax.fori_loop(0, OLD * 6, body, 0)


def refresh_kernel(key_ref, got_ref, free_ref, pos_ref, out_ref):
    own = iota((HALF, QG), 0).astype(F32)
    odd = (iota((HALF, QG), 1) & 1) == 1
    matches = [key_ref[k : k + 1, :] == own for k in range(PER)]
    got = [got_ref[..., k * HALF : (k + 1) * HALF].reshape(QG, HALF) for k in range(PER)]
    for h in range(2):
        cols = slice(h * HALF, (h + 1) * HALF)
        mine = odd if h else ~odd
        placed = jnp.zeros((HALF, HALF), F32)
        for k in range(PER):
            placed += dot(one_hot(matches[k] & mine), got[k])
        out_ref[:, cols] = (free_ref[:, cols].astype(F32) + placed).astype(BF16)


def three_parts(value):
    high = value.astype(BF16).astype(F32)
    rest = value - high
    middle = rest.astype(BF16).astype(F32)
    return [high, middle, rest - middle]


def over_lanes(fn, value):
    total = value[:, :128]
    for at in range(128, value.shape[1], 128):
        total = fn(total, value[:, at : at + 128])
    return total


def score_kernel(
    slot_ref, flag_ref, got_ref, own_ref, other_ref, lab_ref, plane_ref, pos_ref, out_ref,
    own_buf, lab_buf, pos_buf, sems,
):
    rep = lax.axis_index("rep")
    slot = slot_ref[0]
    own_copy = pltpu.make_async_copy(own_ref, own_buf, sems.at[OLD])
    own_copy.start()
    copies = []
    for i in range(OLD):
        source = (i + (i >= slot).astype(jnp.int32)) * D
        copies.append(
            pltpu.make_async_copy(lab_ref.at[pl.ds(source, D), :], lab_buf.at[i], sems.at[i])
        )
        copies[-1].start()
    queries = got_ref[..., ROWS:].reshape(QG, D)
    blocks = [other_ref, own_buf] + [lab_buf.at[i] for i in range(OLD)]

    def logits_of(i):
        if i == 1:
            own_copy.wait()
        elif i > 1:
            copies[i - 2].wait()
        return dot_last(queries, blocks[i][...])

    peak = jnp.full((QG, 1), -jnp.inf, F32)
    total = jnp.zeros((QG, 128), F32)
    grads = jnp.zeros((QG, D), F32)
    following = logits_of(0)
    for i, block in enumerate(blocks):
        logits = following
        if i + 1 < len(blocks):
            following = logits_of(i + 1)
        higher = jnp.maximum(peak, jnp.max(over_lanes(jnp.maximum, logits), axis=1, keepdims=True))
        scale = jnp.exp(peak - higher)
        weight = jnp.exp(logits - higher)
        total = total * scale + over_lanes(jnp.add, weight)
        grads = grads * scale + dot(weight.astype(BF16), block[...])
        peak = higher
    out_ref[..., :D] = grads.astype(BF16).reshape(N_CLS, 2, D)
    pos_buf[...] = pos_ref[...]
    for block, half in ((own_buf, rep), (other_ref, 1 - rep)):
        for part in range(3):
            tile = slot * 6 + half * 3 + part

            @pl.when(flag_ref[0, tile] > 0)
            def _():
                rows = block[part * 128 : (part + 1) * 128, :]
                pos_buf[...] += dot(hits_of(plane_ref, tile * 128), rows)

    positive = pos_buf[...]
    out_ref[..., D : 2 * D] = positive.astype(BF16).reshape(N_CLS, 2, D)
    picked = jnp.sum(queries.astype(F32) * positive, axis=1, keepdims=True)
    exp_total = jnp.sum(total, axis=1, keepdims=True)
    lane = iota((QG, 128), 1)
    stats = jnp.zeros((QG, 128), F32)
    for at, part in enumerate(three_parts(peak) + three_parts(exp_total) + three_parts(picked)):
        stats = jnp.where(lane == at, part, stats)
    out_ref[..., 2 * D :] = stats.astype(BF16).reshape(N_CLS, 2, 128)


def finish_kernel(ids_ref, back_ref, loss_ref, grad_ref):
    back = back_ref[...].reshape(QG, BACK)
    stats = back[:, 2 * D :].astype(F32)

    def column(at):
        return stats[:, at : at + 1] + stats[:, at + 1 : at + 2] + stats[:, at + 2 : at + 3]

    peak, total, picked = column(0), column(3), column(6)
    odd = (iota((QG, 1), 0) & 1) == 1
    valid = jnp.where(ids_ref[lax.axis_index("rep")] >= 0, 1.0, 0.0)
    column_of = iota((4, QG), 1) - 2 * lax.axis_index(CLS)
    losses, grads = [], []
    for h in range(2):
        mine = odd if h else ~odd
        top = jnp.max(jnp.where(mine, peak, -jnp.inf), axis=0, keepdims=True)
        weight = jnp.where(mine, jnp.exp(peak - top), 0.0)
        exp_total = jnp.sum(weight * total, axis=0, keepdims=True)
        count = jnp.sum(jnp.where(column_of == h, valid, 0.0), axis=1, keepdims=True)
        inverse = 1.0 / jnp.sum(count, axis=0, keepdims=True)
        chosen = jnp.sum(jnp.where(mine, picked, 0.0), axis=0, keepdims=True)
        losses.append(top + jnp.log(exp_total) - chosen * inverse)
        scaled = back[:, :D].astype(F32) * (weight / exp_total)
        scaled -= jnp.where(mine, back[:, D : 2 * D].astype(F32), 0.0) * inverse
        grads.append(jnp.sum(scaled, axis=0, keepdims=True))
    loss_ref[...] = jnp.concatenate(losses, axis=1)
    grad_ref[...] = jnp.concatenate(grads, axis=0).astype(BF16).reshape(1, 2, D)


def in_hbm(value):
    return pltpu.with_memory_space_constraint(value, pltpu.HBM)


def per_device(
    queries,
    positives,
    label_vectors,
    refresh_slot,
    features,
    encoder_weight,
    encoder_gain,
    free_vectors,
    targets,
):
    target_rows = targets.reshape(768, 128)
    label_vectors = in_hbm(label_vectors)
    slot = refresh_slot.reshape(1)
    ids = positives.transpose(0, 2, 1)

    sending = pl.pallas_call(
        encode_kernel,
        out_shape=jax.ShapeDtypeStruct((N_CLS, 2, SEND), BF16),
        in_specs=[vmem_spec()] * 5,
        out_specs=vmem_spec(),
        compiler_params=PARAMS,
        name="encode",
    )(features, encoder_weight, encoder_gain.reshape(6, 128), target_rows, queries)
    keys, planes, flags = pl.pallas_call(
        place_kernel,
        out_shape=[
            jax.ShapeDtypeStruct((8, QG), F32),
            jax.ShapeDtypeStruct((4, QG, 128), F32),
            jax.ShapeDtypeStruct((1, 128), jnp.int32),
        ],
        in_specs=[vmem_spec()] * 2,
        out_specs=[vmem_spec()] * 3,
        compiler_params=PARAMS,
        name="place",
    )(target_rows, ids)
    got = lax.all_to_all(sending, CLS, 0, 0, tiled=True)

    any_spec = pl.BlockSpec(memory_space=pl.ANY)
    positive_old = pl.pallas_call(
        positive_kernel,
        out_shape=jax.ShapeDtypeStruct((QG, D), F32),
        in_specs=[smem_spec()] * 2 + [vmem_spec(), any_spec],
        out_specs=vmem_spec(),
        scratch_shapes=[
            pltpu.VMEM((OLD * 6, 128, D), BF16),
            pltpu.SemaphoreType.DMA((OLD * 6,)),
        ],
        compiler_params=PARAMS,
        name="positive",
    )(slot, flags, planes, label_vectors)

    refreshed = pl.pallas_call(
        refresh_kernel,
        out_shape=jax.ShapeDtypeStruct((HALF, D), BF16),
        in_specs=[vmem_spec()] * 3 + [any_spec],
        out_specs=vmem_spec(),
        compiler_params=PARAMS,
        name="refresh",
    )(keys, got, free_vectors, positive_old)
    partner = lax.ppermute(refreshed, "rep", [(0, 1), (1, 0)])

    leaving = pl.pallas_call(
        score_kernel,
        out_shape=jax.ShapeDtypeStruct((N_CLS, 2, BACK), BF16),
        in_specs=[smem_spec()] * 2
        + [vmem_spec(), any_spec, vmem_spec(), any_spec, vmem_spec(), vmem_spec()],
        out_specs=vmem_spec(),
        scratch_shapes=[
            pltpu.VMEM((HALF, D), BF16),
            pltpu.VMEM((OLD, D, D), BF16),
            pltpu.VMEM((QG, D), F32),
            pltpu.SemaphoreType.DMA((SLOTS,)),
        ],
        compiler_params=PARAMS,
        name="score",
    )(slot, flags, got, in_hbm(refreshed), partner, label_vectors, planes, positive_old)
    back = lax.all_to_all(leaving, CLS, 0, 0, tiled=True)
    loss, grads = pl.pallas_call(
        finish_kernel,
        out_shape=[jax.ShapeDtypeStruct((1, 2), F32), jax.ShapeDtypeStruct((1, 2, D), BF16)],
        in_specs=[vmem_spec()] * 2,
        out_specs=[vmem_spec()] * 2,
        compiler_params=PARAMS,
        name="finish",
    )(ids, back)
    return loss, grads, refreshed


def solution(mesh):
    torus = Mesh(
        mesh.devices.reshape(4, 8, 4, mesh.shape["rep"]), ("cls_0", "cls_1", "cls_2", "rep")
    )
    placed = (
        P("rep", CLS, None),
        P(),
        P(CLS, None),
        P(),
        P(CLS_REP, None),
        P(),
        P(),
        P(CLS_REP, None),
        P(),
    )
    return jax.shard_map(
        per_device,
        mesh=torus,
        in_specs=placed,
        out_specs=(P("rep", CLS), P("rep", CLS, None), P(CLS_REP, None)),
        check_vma=False,
    )
```

```python
import jax
import jax.numpy as jnp
from jax import lax
from jax.experimental import pallas as pl
from jax.experimental.pallas import tpu as pltpu
from jax.sharding import Mesh
from jax.sharding import PartitionSpec as P

SLOTS = 8
OLD = SLOTS - 1
D = 768
HALF = 384
QG = 256
N_CLS = 128
PER = 3
CLS = ("cls_0", "cls_1", "cls_2")
CLS_REP = ("cls_0", "cls_1", "cls_2", "rep")
ROWS = PER * HALF
SEND = ROWS + D
BACK = 2 * D + 128
F32 = jnp.float32
BF16 = jnp.bfloat16
PARAMS = pltpu.CompilerParams(vmem_limit_bytes=24 * 1024 * 1024)


def vmem_spec():
    return pl.BlockSpec(memory_space=pltpu.VMEM)


def smem_spec():
    return pl.BlockSpec(memory_space=pltpu.SMEM)


def iota(shape, dim):
    return lax.broadcasted_iota(jnp.int32, shape, dim)


def dot(a, b):
    return jnp.dot(a, b, preferred_element_type=F32)


def dot_last(a, b):
    return lax.dot_general(a, b, (((1,), (1,)), ((), ())), preferred_element_type=F32)


def dot_first(a, b):
    return lax.dot_general(a, b, (((0,), (0,)), ((), ())), preferred_element_type=F32)


def one_hot(mask):
    return jnp.where(mask, 1.0, 0.0).astype(BF16)


def spread_down(row):
    return jnp.broadcast_to(row, (128, 128)).T


def encode_kernel(
    feat_ref, weight_ref, gain_ref, tgt_ref, q_ref, out_ref,
    feat_buf, weight_buf, gain_buf, tgt_buf, q_buf, sems,
):
    row = 3 * lax.axis_index(CLS_REP)
    begin = pl.multiple_of(jnp.minimum(row // 8 * 8, 768 - 16), 8)
    pairs = [
        (tgt_ref.at[pl.ds(begin, 16), :], tgt_buf), (q_ref, q_buf), (weight_ref, weight_buf),
        (feat_ref, feat_buf), (gain_ref, gain_buf),
    ]
    copies = [pltpu.make_async_copy(a, b, sems.at[i]) for i, (a, b) in enumerate(pairs)]
    for copy in copies:
        copy.start()
    copies[0].wait()
    rows = [tgt_buf[pl.ds(row - begin + a, 1), :].astype(F32) for a in range(3)]
    columns = [spread_down(row) for row in rows]
    ranks = []
    for row in rows:
        rank = jnp.zeros((1, 128), F32)
        for column in columns:
            rank += jnp.sum(jnp.where(column < row, 1.0, 0.0), axis=0, keepdims=True)
        ranks.append(rank)
    rank = jnp.concatenate(ranks, axis=1)
    line = iota((QG, HALF), 0)
    first = ((line >> 1) * PER).astype(F32)
    odd = (line & 1) == 1
    chosen = []
    for k in range(PER):
        hit = rank == first + float(k)
        chosen.append((one_hot(hit & ~odd), one_hot(hit & odd)))
    copies[1].wait()
    out_ref[..., ROWS:] = jnp.broadcast_to(q_buf[...], (N_CLS, 2, D))
    for copy in copies[2:]:
        copy.wait()
    hidden = dot(feat_buf[...], weight_buf[...])
    mean = jnp.mean(hidden * hidden, axis=1, keepdims=True)
    gain = jnp.concatenate([gain_buf[i : i + 1, :] for i in range(6)], axis=1)
    encoded = (hidden * lax.rsqrt(mean + 1e-06) * gain).astype(BF16)
    for k, (even_rows, odd_rows) in enumerate(chosen):
        total = dot(even_rows, encoded[:, :HALF]) + dot(odd_rows, encoded[:, HALF:])
        out_ref[..., k * HALF : (k + 1) * HALF] = total.astype(BF16).reshape(N_CLS, 2, HALF)


def place_kernel(tgt_ref, ids_ref, key_ref, plane_ref, flag_ref):
    cls_index, rep_index = lax.axis_index(CLS), lax.axis_index("rep")
    base = cls_index * (2 * HALF) + rep_index * HALF
    parts = [tgt_ref[pl.ds(3 * rep_index + a, N_CLS, stride=6), :] for a in range(3)]
    offsets = jnp.concatenate(parts, axis=1) - base
    inside = (offsets >= 0) & (offsets < HALF)
    far = 4096.0
    keys = jnp.where(inside, offsets.astype(F32), far)
    source = iota((N_CLS, QG), 0)
    twice = (iota((N_CLS, QG), 1) >> 1) == source
    for k in range(PER):
        least = jnp.min(keys, axis=1, keepdims=True)
        keys = jnp.where(keys == least, far, keys)
        wide = jnp.broadcast_to(least, (N_CLS, QG))
        key_ref[k : k + 1, :] = jnp.sum(jnp.where(twice, wide, 0.0), axis=0, keepdims=True)
    first = cls_index * (SLOTS * D)
    lane = iota((QG, 128), 1)
    seen = jnp.zeros((QG, 128), F32)
    for k in range(4):
        own = (ids_ref[rep_index, k : k + 1, :] - first).astype(F32)
        plane = jnp.concatenate([spread_down(own[:, :128]), spread_down(own[:, 128:])], axis=0)
        plane_ref[k] = plane
        seen = jnp.where((plane.astype(jnp.int32) >> 7) == lane, 1.0, seen)
    flag_ref[...] = jnp.max(seen, axis=0, keepdims=True).astype(jnp.int32)


def hits_of(plane_ref, first):
    label = iota((QG, 128), 1).astype(F32) + first.astype(F32)
    hits = jnp.zeros((QG, 128), F32)
    for k in range(4):
        hits += jnp.where(plane_ref[k] == label, 1.0, 0.0)
    return hits.astype(BF16)


def positive_kernel(slot_ref, flag_ref, plane_ref, lab_ref, out_ref, lab_buf, sems):
    out_ref[...] = jnp.zeros_like(out_ref)

    def copy_of(i, part):
        tile = (i + (i >= slot_ref[0]).astype(jnp.int32)) * 6 + part
        at = i * 6 + part
        return tile, pltpu.make_async_copy(
            lab_ref.at[pl.ds(tile * 128, 128), :], lab_buf.at[at], sems.at[at]
        )

    for i in range(OLD):
        for part in range(6):
            tile, copy = copy_of(i, part)
            pl.when(flag_ref[0, tile] > 0)(copy.start)

    def body(at, carry):
        i = at // 6
        tile, copy = copy_of(i, at - i * 6)

        @pl.when(flag_ref[0, tile] > 0)
        def _():
            copy.wait()
            out_ref[...] += dot(hits_of(plane_ref, tile * 128), lab_buf[at])

        return carry

    lax.fori_loop(0, OLD * 6, body, 0)


def refresh_kernel(key_ref, got_ref, free_ref, pos_ref, out_ref):
    own = iota((HALF, QG), 0).astype(F32)
    odd = (iota((HALF, QG), 1) & 1) == 1
    matches = [key_ref[k : k + 1, :] == own for k in range(PER)]
    got = [got_ref[..., k * HALF : (k + 1) * HALF].reshape(QG, HALF) for k in range(PER)]
    for h in range(2):
        cols = slice(h * HALF, (h + 1) * HALF)
        mine = odd if h else ~odd
        placed = jnp.zeros((HALF, HALF), F32)
        for k in range(PER):
            placed += dot(one_hot(matches[k] & mine), got[k])
        out_ref[:, cols] = (free_ref[:, cols].astype(F32) + placed).astype(BF16)


def three_parts(value):
    high = value.astype(BF16).astype(F32)
    rest = value - high
    middle = rest.astype(BF16).astype(F32)
    return [high, middle, rest - middle]


def over_lanes(fn, value):
    total = value[:, :128]
    for at in range(128, value.shape[1], 128):
        total = fn(total, value[:, at : at + 128])
    return total


def absorb_all(state, queries, blocks, waits):
    peak, total, grads = state

    def logits_of(i):
        for copy in waits[i]:
            copy.wait()
        return dot_last(queries, blocks[i][...])

    following = logits_of(0)
    for i, block in enumerate(blocks):
        logits = following
        if i + 1 < len(blocks):
            following = logits_of(i + 1)
        higher = jnp.maximum(peak, jnp.max(over_lanes(jnp.maximum, logits), axis=1, keepdims=True))
        scale = jnp.exp(peak - higher)
        weight = jnp.exp(logits - higher)
        total = total * scale + over_lanes(jnp.add, weight)
        grads = grads * scale + dot(weight.astype(BF16), block[...])
        peak = higher
    return peak, total, grads


def old_kernel(
    slot_ref, got_ref, own_ref, lab_ref, peak_ref, total_ref, grad_ref, own_buf, lab_buf, sems
):
    slot = slot_ref[0]
    own_copy = pltpu.make_async_copy(own_ref, own_buf, sems.at[OLD])
    own_copy.start()
    copies = []
    for i in range(OLD):
        source = (i + (i >= slot).astype(jnp.int32)) * D
        copies.append(
            pltpu.make_async_copy(lab_ref.at[pl.ds(source, D), :], lab_buf.at[i], sems.at[i])
        )
        copies[-1].start()
    start = (jnp.full((QG, 1), -jnp.inf, F32), jnp.zeros((QG, 128), F32), jnp.zeros((QG, D), F32))
    peak, total, grads = absorb_all(
        start,
        got_ref[..., ROWS:].reshape(QG, D),
        [own_buf] + [lab_buf.at[i] for i in range(OLD)],
        [[own_copy]] + [[copy] for copy in copies],
    )
    peak_ref[...] = jnp.broadcast_to(peak, (QG, 128))
    total_ref[...] = total
    grad_ref[...] = grads


def score_kernel(
    slot_ref, flag_ref, got_ref, own_ref, other_ref, peak_ref, total_ref, grad_ref, plane_ref,
    pos_ref, out_ref, own_buf, pos_buf, sem,
):
    rep = lax.axis_index("rep")
    slot = slot_ref[0]
    own_copy = pltpu.make_async_copy(own_ref, own_buf, sem)
    own_copy.start()
    queries = got_ref[..., ROWS:].reshape(QG, D)
    state = (peak_ref[:, :1], total_ref[...], grad_ref[...])
    peak, total, grads = absorb_all(state, queries, [other_ref], [[]])
    out_ref[..., :D] = grads.astype(BF16).reshape(N_CLS, 2, D)
    pos_buf[...] = pos_ref[...]
    own_copy.wait()
    for block, half in ((own_buf, rep), (other_ref, 1 - rep)):
        for part in range(3):
            tile = slot * 6 + half * 3 + part

            @pl.when(flag_ref[0, tile] > 0)
            def _():
                rows = block[part * 128 : (part + 1) * 128, :]
                pos_buf[...] += dot(hits_of(plane_ref, tile * 128), rows)

    positive = pos_buf[...]
    out_ref[..., D : 2 * D] = positive.astype(BF16).reshape(N_CLS, 2, D)
    picked = jnp.sum(queries.astype(F32) * positive, axis=1, keepdims=True)
    exp_total = jnp.sum(total, axis=1, keepdims=True)
    lane = iota((QG, 128), 1)
    stats = jnp.zeros((QG, 128), F32)
    for at, part in enumerate(three_parts(peak) + three_parts(exp_total) + three_parts(picked)):
        stats = jnp.where(lane == at, part, stats)
    out_ref[..., 2 * D :] = stats.astype(BF16).reshape(N_CLS, 2, 128)


def finish_kernel(ids_ref, back_ref, loss_ref, grad_ref):
    back = back_ref[...].reshape(QG, BACK)
    stats = back[:, 2 * D :].astype(F32)

    def column(at):
        return stats[:, at : at + 1] + stats[:, at + 1 : at + 2] + stats[:, at + 2 : at + 3]

    peak, total, picked = column(0), column(3), column(6)
    odd = (iota((QG, 1), 0) & 1) == 1
    valid = jnp.where(ids_ref[lax.axis_index("rep")] >= 0, 1.0, 0.0)
    column_of = iota((4, QG), 1) - 2 * lax.axis_index(CLS)
    losses, grads = [], []
    for h in range(2):
        mine = odd if h else ~odd
        top = jnp.max(jnp.where(mine, peak, -jnp.inf), axis=0, keepdims=True)
        weight = jnp.where(mine, jnp.exp(peak - top), 0.0)
        exp_total = jnp.sum(weight * total, axis=0, keepdims=True)
        count = jnp.sum(jnp.where(column_of == h, valid, 0.0), axis=1, keepdims=True)
        inverse = 1.0 / jnp.sum(count, axis=0, keepdims=True)
        chosen = jnp.sum(jnp.where(mine, picked, 0.0), axis=0, keepdims=True)
        losses.append(top + jnp.log(exp_total) - chosen * inverse)
        scaled = back[:, :D].astype(F32) * (weight / exp_total)
        scaled -= jnp.where(mine, back[:, D : 2 * D].astype(F32), 0.0) * inverse
        grads.append(jnp.sum(scaled, axis=0, keepdims=True))
    loss_ref[...] = jnp.concatenate(losses, axis=1)
    grad_ref[...] = jnp.concatenate(grads, axis=0).astype(BF16).reshape(1, 2, D)


def in_hbm(value):
    return pltpu.with_memory_space_constraint(value, pltpu.HBM)


def per_device(
    queries,
    positives,
    label_vectors,
    refresh_slot,
    features,
    encoder_weight,
    encoder_gain,
    free_vectors,
    targets,
):
    target_rows = targets.reshape(768, 128)
    label_vectors = in_hbm(label_vectors)
    slot = refresh_slot.reshape(1)
    ids = positives.transpose(0, 2, 1)

    any_spec = pl.BlockSpec(memory_space=pl.ANY)
    sending = pl.pallas_call(
        encode_kernel,
        out_shape=jax.ShapeDtypeStruct((N_CLS, 2, SEND), BF16),
        in_specs=[any_spec] * 5,
        out_specs=vmem_spec(),
        scratch_shapes=[
            pltpu.VMEM((HALF, D), BF16),
            pltpu.VMEM((D, D), BF16),
            pltpu.VMEM((6, 128), F32),
            pltpu.VMEM((16, 128), jnp.int32),
            pltpu.VMEM((1, 2, D), BF16),
            pltpu.SemaphoreType.DMA((5,)),
        ],
        compiler_params=PARAMS,
        name="encode",
    )(
        in_hbm(features),
        in_hbm(encoder_weight),
        in_hbm(encoder_gain.reshape(6, 128)),
        in_hbm(target_rows),
        in_hbm(queries),
    )
    keys, planes, flags = pl.pallas_call(
        place_kernel,
        out_shape=[
            jax.ShapeDtypeStruct((8, QG), F32),
            jax.ShapeDtypeStruct((4, QG, 128), F32),
            jax.ShapeDtypeStruct((1, 128), jnp.int32),
        ],
        in_specs=[vmem_spec()] * 2,
        out_specs=[vmem_spec()] * 3,
        compiler_params=PARAMS,
        name="place",
    )(target_rows, ids)
    got = lax.all_to_all(sending, CLS, 0, 0, tiled=True)

    positive_old = pl.pallas_call(
        positive_kernel,
        out_shape=jax.ShapeDtypeStruct((QG, D), F32),
        in_specs=[smem_spec()] * 2 + [vmem_spec(), any_spec],
        out_specs=vmem_spec(),
        scratch_shapes=[
            pltpu.VMEM((OLD * 6, 128, D), BF16),
            pltpu.SemaphoreType.DMA((OLD * 6,)),
        ],
        compiler_params=PARAMS,
        name="positive",
    )(slot, flags, planes, label_vectors)

    refreshed = pl.pallas_call(
        refresh_kernel,
        out_shape=jax.ShapeDtypeStruct((HALF, D), BF16),
        in_specs=[vmem_spec()] * 3 + [any_spec],
        out_specs=vmem_spec(),
        compiler_params=PARAMS,
        name="refresh",
    )(keys, got, free_vectors, positive_old)
    partner = lax.ppermute(refreshed, "rep", [(0, 1), (1, 0)])

    own = in_hbm(refreshed)
    state = pl.pallas_call(
        old_kernel,
        out_shape=[
            jax.ShapeDtypeStruct((QG, 128), F32),
            jax.ShapeDtypeStruct((QG, 128), F32),
            jax.ShapeDtypeStruct((QG, D), F32),
        ],
        in_specs=[smem_spec(), vmem_spec(), any_spec, any_spec],
        out_specs=[vmem_spec()] * 3,
        scratch_shapes=[
            pltpu.VMEM((HALF, D), BF16),
            pltpu.VMEM((OLD, D, D), BF16),
            pltpu.SemaphoreType.DMA((SLOTS,)),
        ],
        compiler_params=PARAMS,
        name="old",
    )(slot, got, own, label_vectors)
    partner, *state = lax.optimization_barrier((partner, *state))
    leaving = pl.pallas_call(
        score_kernel,
        out_shape=jax.ShapeDtypeStruct((N_CLS, 2, BACK), BF16),
        in_specs=[smem_spec()] * 2 + [vmem_spec(), any_spec] + [vmem_spec()] * 6,
        out_specs=vmem_spec(),
        scratch_shapes=[
            pltpu.VMEM((HALF, D), BF16),
            pltpu.VMEM((QG, D), F32),
            pltpu.SemaphoreType.DMA,
        ],
        compiler_params=PARAMS,
        name="score",
    )(slot, flags, got, own, partner, *state, planes, positive_old)
    back = lax.all_to_all(leaving, CLS, 0, 0, tiled=True)
    loss, grads = pl.pallas_call(
        finish_kernel,
        out_shape=[jax.ShapeDtypeStruct((1, 2), F32), jax.ShapeDtypeStruct((1, 2, D), BF16)],
        in_specs=[vmem_spec()] * 2,
        out_specs=[vmem_spec()] * 2,
        compiler_params=PARAMS,
        name="finish",
    )(ids, back)
    return loss, grads, refreshed


def solution(mesh):
    torus = Mesh(
        mesh.devices.reshape(4, 8, 4, mesh.shape["rep"]), ("cls_0", "cls_1", "cls_2", "rep")
    )
    placed = (
        P("rep", CLS, None),
        P(),
        P(CLS, None),
        P(),
        P(CLS_REP, None),
        P(),
        P(),
        P(CLS_REP, None),
        P(),
    )
    return jax.shard_map(
        per_device,
        mesh=torus,
        in_specs=placed,
        out_specs=(P("rep", CLS), P("rep", CLS, None), P(CLS_REP, None)),
        check_vma=False,
    )
```

```python
import jax
import jax.numpy as jnp
from jax import lax
from jax.experimental import pallas as pl
from jax.experimental.pallas import tpu as pltpu
from jax.sharding import Mesh
from jax.sharding import PartitionSpec as P

SLOTS = 8
OLD = SLOTS - 1
D = 768
HALF = 384
QG = 256
N_CLS = 128
PER = 3
CLS = ("cls_0", "cls_1", "cls_2")
CLS_REP = ("cls_0", "cls_1", "cls_2", "rep")
ROWS = PER * HALF
SEND = ROWS + D
QUARTER = 192
BACK = D + 256
F32 = jnp.float32
BF16 = jnp.bfloat16
PARAMS = pltpu.CompilerParams(vmem_limit_bytes=24 * 1024 * 1024)


def vmem_spec():
    return pl.BlockSpec(memory_space=pltpu.VMEM)


def smem_spec():
    return pl.BlockSpec(memory_space=pltpu.SMEM)


def iota(shape, dim):
    return lax.broadcasted_iota(jnp.int32, shape, dim)


def dot(a, b):
    return jnp.dot(a, b, preferred_element_type=F32)


def dot_last(a, b):
    return lax.dot_general(a, b, (((1,), (1,)), ((), ())), preferred_element_type=F32)


def dot_first(a, b):
    return lax.dot_general(a, b, (((0,), (0,)), ((), ())), preferred_element_type=F32)


def one_hot(mask):
    return jnp.where(mask, 1.0, 0.0).astype(BF16)


def spread_down(row):
    return jnp.broadcast_to(row, (128, 128)).T


def own_target_rows():
    row = 3 * lax.axis_index(CLS_REP)
    return row, pl.multiple_of(jnp.minimum(row // 8 * 8, 768 - 16), 8)


def encode_kernel(
    feat_ref, weight_ref, gain_ref, tgt_ref, q_ref, out_ref, row_ref,
    feat_buf, weight_buf, gain_buf, tgt_buf, q_buf, sems,
):
    row, begin = own_target_rows()
    pairs = [
        (tgt_ref.at[pl.ds(begin, 16), :], tgt_buf), (q_ref, q_buf), (weight_ref, weight_buf),
        (feat_ref, feat_buf), (gain_ref, gain_buf),
    ]
    copies = [pltpu.make_async_copy(a, b, sems.at[i]) for i, (a, b) in enumerate(pairs)]
    for copy in copies:
        copy.start()
    copies[0].wait()
    rows = [tgt_buf[pl.ds(row - begin + a, 1), :].astype(F32) for a in range(3)]
    columns = [spread_down(row) for row in rows]
    ranks = []
    for row in rows:
        rank = jnp.zeros((1, 128), F32)
        for column in columns:
            rank += jnp.sum(jnp.where(column < row, 1.0, 0.0), axis=0, keepdims=True)
        ranks.append(rank)
    rank = jnp.concatenate(ranks, axis=1)
    line = iota((QG, HALF), 0)
    first = ((line >> 1) * PER).astype(F32)
    odd = (line & 1) == 1
    chosen = []
    for k in range(PER):
        hit = rank == first + float(k)
        chosen.append((one_hot(hit & ~odd), one_hot(hit & odd)))
    copies[1].wait()
    out_ref[..., ROWS:] = jnp.broadcast_to(q_buf[...], (N_CLS, 2, D))
    for copy in copies[2:]:
        copy.wait()
    hidden = dot(feat_buf[...], weight_buf[...])
    mean = jnp.mean(hidden * hidden, axis=1, keepdims=True)
    gain = jnp.concatenate([gain_buf[i : i + 1, :] for i in range(6)], axis=1)
    encoded = (hidden * lax.rsqrt(mean + 1e-06) * gain).astype(BF16)
    row_ref[...] = encoded
    for k, (even_rows, odd_rows) in enumerate(chosen):
        total = dot(even_rows, encoded[:, :HALF]) + dot(odd_rows, encoded[:, HALF:])
        out_ref[..., k * HALF : (k + 1) * HALF] = total.astype(BF16).reshape(N_CLS, 2, HALF)


def place_kernel(tgt_ref, ids_ref, key_ref, plane_ref, flag_ref, across_ref):
    cls_index, rep_index = lax.axis_index(CLS), lax.axis_index("rep")
    base = cls_index * (2 * HALF) + rep_index * HALF
    parts = [tgt_ref[pl.ds(3 * rep_index + a, N_CLS, stride=6), :] for a in range(3)]
    offsets = jnp.concatenate(parts, axis=1) - base
    inside = (offsets >= 0) & (offsets < HALF)
    far = 4096.0
    keys = jnp.where(inside, offsets.astype(F32), far)
    source = iota((N_CLS, QG), 0)
    twice = (iota((N_CLS, QG), 1) >> 1) == source
    for k in range(PER):
        least = jnp.min(keys, axis=1, keepdims=True)
        keys = jnp.where(keys == least, far, keys)
        wide = jnp.broadcast_to(least, (N_CLS, QG))
        key_ref[k : k + 1, :] = jnp.sum(jnp.where(twice, wide, 0.0), axis=0, keepdims=True)
    first = cls_index * (SLOTS * D)
    lane = iota((QG, 128), 1)
    seen = jnp.zeros((QG, 128), F32)

    def plane_of(half, k):
        own = (ids_ref[half, k : k + 1, :] - first).astype(F32)
        return jnp.concatenate([spread_down(own[:, :128]), spread_down(own[:, 128:])], axis=0)

    for k in range(4):
        across_ref[k] = plane_of(1 - rep_index, k)
        plane = plane_of(rep_index, k)
        plane_ref[k] = plane
        seen = jnp.where((plane.astype(jnp.int32) >> 7) == lane, 1.0, seen)
    flag_ref[...] = jnp.max(seen, axis=0, keepdims=True).astype(jnp.int32)


def hits_at(plane_ref, label):
    hits = jnp.zeros((QG, 128), F32)
    for k in range(4):
        hits += jnp.where(plane_ref[k] == label, 1.0, 0.0)
    return hits.astype(BF16)


def hits_of(plane_ref, first):
    return hits_at(plane_ref, iota((QG, 128), 1).astype(F32) + first.astype(F32))


def positive_kernel(slot_ref, flag_ref, plane_ref, lab_ref, out_ref, lab_buf, sems):
    out_ref[...] = jnp.zeros_like(out_ref)

    def copy_of(i, part):
        tile = (i + (i >= slot_ref[0]).astype(jnp.int32)) * 6 + part
        at = i * 6 + part
        return tile, pltpu.make_async_copy(
            lab_ref.at[pl.ds(tile * 128, 128), :], lab_buf.at[at], sems.at[at]
        )

    for i in range(OLD):
        for part in range(6):
            tile, copy = copy_of(i, part)
            pl.when(flag_ref[0, tile] > 0)(copy.start)

    def body(at, carry):
        i = at // 6
        tile, copy = copy_of(i, at - i * 6)

        @pl.when(flag_ref[0, tile] > 0)
        def _():
            copy.wait()
            out_ref[...] += dot(hits_of(plane_ref, tile * 128), lab_buf[at])

        return carry

    lax.fori_loop(0, OLD * 6, body, 0)


def share_kernel(
    slot_ref, tgt_ref, free_ref, row_ref, plane_ref, across_ref, here_ref, there_ref, tgt_buf, sem
):
    row, begin = own_target_rows()
    copy = pltpu.make_async_copy(tgt_ref.at[pl.ds(begin, 16), :], tgt_buf, sem)
    copy.start()
    slot_first = slot_ref[0] * D
    free_first = slot_first + lax.axis_index("rep") * HALF
    copy.wait()
    labels = []
    for part in range(3):
        target = tgt_buf[pl.ds(row - begin + part, 1), :]
        owner = ((target >> 8) * 21846) >> 16
        behind = owner - lax.axis_index(CLS)
        local = behind * (SLOTS * D) + slot_first + (target - owner * D)
        labels.append(local.astype(F32))
    for planes, out_ref in ((plane_ref, here_ref), (across_ref, there_ref)):
        total = jnp.zeros((QG, D), F32)
        for part in range(3):
            rows = slice(part * 128, (part + 1) * 128)
            total += dot(hits_of(planes, free_first + part * 128), free_ref[rows, :])
            total += dot(hits_at(planes, labels[part]), row_ref[rows, :])
        out_ref[...] = total.astype(out_ref.dtype)


def quarter_kernel(old_ref, here_ref, came_ref, *out_refs):
    total = (old_ref[...] + here_ref[...] + came_ref[...].astype(F32)).astype(BF16)
    line, lane = iota((D, 256), 0), iota((D, 256), 1)
    for shift, out_ref in enumerate(out_refs):
        first = ((lax.axis_index("cls_2") + shift) & 3) * QUARTER
        pick = one_hot((line == first + lane) & (lane < QUARTER))
        out_ref[...] = dot(total, pick).astype(BF16)


def refresh_kernel(key_ref, got_ref, free_ref, *refs):
    out_ref = refs[-1]
    own = iota((HALF, QG), 0).astype(F32)
    odd = (iota((HALF, QG), 1) & 1) == 1
    matches = [key_ref[k : k + 1, :] == own for k in range(PER)]
    got = [got_ref[..., k * HALF : (k + 1) * HALF].reshape(QG, HALF) for k in range(PER)]
    for h in range(2):
        cols = slice(h * HALF, (h + 1) * HALF)
        mine = odd if h else ~odd
        placed = jnp.zeros((HALF, HALF), F32)
        for k in range(PER):
            placed += dot(one_hot(matches[k] & mine), got[k])
        out_ref[:, cols] = (free_ref[:, cols].astype(F32) + placed).astype(BF16)


def three_parts(value):
    high = value.astype(BF16).astype(F32)
    rest = value - high
    middle = rest.astype(BF16).astype(F32)
    return [high, middle, rest - middle]


def over_lanes(fn, value):
    total = value[:, :128]
    for at in range(128, value.shape[1], 128):
        total = fn(total, value[:, at : at + 128])
    return total


def absorb_all(state, queries, blocks, waits):
    peak, total, grads = state

    def logits_of(i):
        for copy in waits[i]:
            copy.wait()
        return dot_last(queries, blocks[i][...])

    following = logits_of(0)
    for i, block in enumerate(blocks):
        logits = following
        if i + 1 < len(blocks):
            following = logits_of(i + 1)
        higher = jnp.maximum(peak, jnp.max(over_lanes(jnp.maximum, logits), axis=1, keepdims=True))
        scale = jnp.exp(peak - higher)
        weight = jnp.exp(logits - higher)
        total = total * scale + over_lanes(jnp.add, weight)
        grads = grads * scale + dot(weight.astype(BF16), block[...])
        peak = higher
    return peak, total, grads


def old_kernel(
    slot_ref, got_ref, own_ref, lab_ref, peak_ref, total_ref, grad_ref, own_buf, lab_buf, sems
):
    slot = slot_ref[0]
    own_copy = pltpu.make_async_copy(own_ref, own_buf, sems.at[OLD])
    own_copy.start()
    copies = []
    for i in range(OLD):
        source = (i + (i >= slot).astype(jnp.int32)) * D
        copies.append(
            pltpu.make_async_copy(lab_ref.at[pl.ds(source, D), :], lab_buf.at[i], sems.at[i])
        )
        copies[-1].start()
    start = (jnp.full((QG, 1), -jnp.inf, F32), jnp.zeros((QG, 128), F32), jnp.zeros((QG, D), F32))
    peak, total, grads = absorb_all(
        start,
        got_ref[..., ROWS:].reshape(QG, D),
        [own_buf] + [lab_buf.at[i] for i in range(OLD)],
        [[own_copy]] + [[copy] for copy in copies],
    )
    peak_ref[...] = jnp.broadcast_to(peak, (QG, 128))
    total_ref[...] = total
    grad_ref[...] = grads


def score_kernel(
    slot_ref, flag_ref, got_ref, own_ref, other_ref, peak_ref, total_ref, grad_ref, plane_ref,
    pos_ref, *refs
):
    quarter_refs, (out_ref, own_buf, pos_buf, sem) = refs[:4], refs[4:]
    rep = lax.axis_index("rep")
    slot = slot_ref[0]
    own_copy = pltpu.make_async_copy(own_ref, own_buf, sem)
    own_copy.start()
    queries = got_ref[..., ROWS:].reshape(QG, D)
    state = (peak_ref[:, :1], total_ref[...], grad_ref[...])
    peak, total, grads = absorb_all(state, queries, [other_ref], [[]])
    out_ref[..., :D] = grads.astype(BF16).reshape(N_CLS, 2, D)
    pos_buf[...] = pos_ref[...]
    own_copy.wait()
    for block, half in ((own_buf, rep), (other_ref, 1 - rep)):
        for part in range(3):
            tile = slot * 6 + half * 3 + part

            @pl.when(flag_ref[0, tile] > 0)
            def _():
                rows = block[part * 128 : (part + 1) * 128, :]
                pos_buf[...] += dot(hits_of(plane_ref, tile * 128), rows)

    positive = pos_buf[...]
    picked = jnp.sum(queries.astype(F32) * positive, axis=1, keepdims=True)
    exp_total = jnp.sum(total, axis=1, keepdims=True)
    lane = iota((QG, 256), 1)
    tail = sum(ref[...].astype(F32) for ref in quarter_refs)
    for at, part in enumerate(three_parts(peak) + three_parts(exp_total) + three_parts(picked)):
        tail = jnp.where(lane == QUARTER + at, part, tail)
    out_ref[..., D:] = tail.astype(BF16).reshape(N_CLS, 2, 256)


def finish_kernel(ids_ref, back_ref, loss_ref, grad_ref):
    back = back_ref[...].reshape(QG, BACK)
    tail = back[:, D:].astype(F32)
    stats = tail[:, 128:]

    def column(at):
        at += QUARTER - 128
        return stats[:, at : at + 1] + stats[:, at + 1 : at + 2] + stats[:, at + 2 : at + 3]

    peak, total, picked = column(0), column(3), column(6)
    odd = (iota((QG, 1), 0) & 1) == 1
    ring = (iota((QG, 1), 0) >> 1) & 3
    valid = jnp.where(ids_ref[lax.axis_index("rep")] >= 0, 1.0, 0.0)
    column_of = iota((4, QG), 1) - 2 * lax.axis_index(CLS)
    losses, grads = [], []
    for h in range(2):
        mine = odd if h else ~odd
        top = jnp.max(jnp.where(mine, peak, -jnp.inf), axis=0, keepdims=True)
        weight = jnp.where(mine, jnp.exp(peak - top), 0.0)
        exp_total = jnp.sum(weight * total, axis=0, keepdims=True)
        count = jnp.sum(jnp.where(column_of == h, valid, 0.0), axis=1, keepdims=True)
        inverse = 1.0 / jnp.sum(count, axis=0, keepdims=True)
        chosen = jnp.sum(jnp.where(mine, picked, 0.0), axis=0, keepdims=True)
        losses.append(top + jnp.log(exp_total) - chosen * inverse)
        scaled = back[:, :D].astype(F32) * (weight / exp_total)
        parts = []
        for x in range(4):
            from_x = jnp.where(mine & (ring == x), tail[:, :QUARTER], 0.0)
            parts.append(jnp.sum(from_x, axis=0, keepdims=True))
        positive = jnp.concatenate(parts, axis=1)
        grads.append(jnp.sum(scaled, axis=0, keepdims=True) - positive * inverse)
    loss_ref[...] = jnp.concatenate(losses, axis=1)
    grad_ref[...] = jnp.concatenate(grads, axis=0).astype(BF16).reshape(1, 2, D)


def in_hbm(value):
    return pltpu.with_memory_space_constraint(value, pltpu.HBM)


def per_device(
    queries,
    positives,
    label_vectors,
    refresh_slot,
    features,
    encoder_weight,
    encoder_gain,
    free_vectors,
    targets,
):
    target_rows = targets.reshape(768, 128)
    label_vectors = in_hbm(label_vectors)
    slot = refresh_slot.reshape(1)
    ids = positives.transpose(0, 2, 1)

    any_spec = pl.BlockSpec(memory_space=pl.ANY)
    sending, encoded = pl.pallas_call(
        encode_kernel,
        out_shape=[
            jax.ShapeDtypeStruct((N_CLS, 2, SEND), BF16),
            jax.ShapeDtypeStruct((HALF, D), BF16),
        ],
        in_specs=[any_spec] * 5,
        out_specs=[vmem_spec()] * 2,
        scratch_shapes=[
            pltpu.VMEM((HALF, D), BF16),
            pltpu.VMEM((D, D), BF16),
            pltpu.VMEM((6, 128), F32),
            pltpu.VMEM((16, 128), jnp.int32),
            pltpu.VMEM((1, 2, D), BF16),
            pltpu.SemaphoreType.DMA((5,)),
        ],
        compiler_params=PARAMS,
        name="encode",
    )(
        in_hbm(features),
        in_hbm(encoder_weight),
        in_hbm(encoder_gain.reshape(6, 128)),
        in_hbm(target_rows),
        in_hbm(queries),
    )
    keys, planes, flags, across = pl.pallas_call(
        place_kernel,
        out_shape=[
            jax.ShapeDtypeStruct((8, QG), F32),
            jax.ShapeDtypeStruct((4, QG, 128), F32),
            jax.ShapeDtypeStruct((1, 128), jnp.int32),
            jax.ShapeDtypeStruct((4, QG, 128), F32),
        ],
        in_specs=[vmem_spec()] * 2,
        out_specs=[vmem_spec()] * 4,
        compiler_params=PARAMS,
        name="place",
    )(target_rows, ids)
    got = lax.all_to_all(sending, CLS, 0, 0, tiled=True)

    positive_old = pl.pallas_call(
        positive_kernel,
        out_shape=jax.ShapeDtypeStruct((QG, D), F32),
        in_specs=[smem_spec()] * 2 + [vmem_spec(), any_spec],
        out_specs=vmem_spec(),
        scratch_shapes=[
            pltpu.VMEM((OLD * 6, 128, D), BF16),
            pltpu.SemaphoreType.DMA((OLD * 6,)),
        ],
        compiler_params=PARAMS,
        name="positive",
    )(slot, flags, planes, label_vectors)

    here, there = pl.pallas_call(
        share_kernel,
        out_shape=[jax.ShapeDtypeStruct((QG, D), F32), jax.ShapeDtypeStruct((QG, D), BF16)],
        in_specs=[smem_spec(), any_spec] + [vmem_spec()] * 4,
        out_specs=[vmem_spec()] * 2,
        scratch_shapes=[pltpu.VMEM((16, 128), jnp.int32), pltpu.SemaphoreType.DMA],
        compiler_params=PARAMS,
        name="share",
    )(slot, in_hbm(target_rows), free_vectors, encoded, planes, across)
    came = lax.ppermute(there, "rep", [(0, 1), (1, 0)])
    quarters = pl.pallas_call(
        quarter_kernel,
        out_shape=[jax.ShapeDtypeStruct((QG, 256), BF16)] * 4,
        in_specs=[vmem_spec()] * 3,
        out_specs=[vmem_spec()] * 4,
        compiler_params=PARAMS,
        name="quarter",
    )(positive_old, here, came)
    along_x = [quarters[0]] + [
        lax.ppermute(quarters[shift], "cls_2", [(x, (x + shift) % 4) for x in range(4)])
        for shift in (1, 2, 3)
    ]

    refreshed = pl.pallas_call(
        refresh_kernel,
        out_shape=jax.ShapeDtypeStruct((HALF, D), BF16),
        in_specs=[vmem_spec()] * 3 + [any_spec] * 4,
        out_specs=vmem_spec(),
        compiler_params=PARAMS,
        name="refresh",
    )(keys, got, free_vectors, *along_x)
    partner = lax.ppermute(refreshed, "rep", [(0, 1), (1, 0)])

    own = in_hbm(refreshed)
    state = pl.pallas_call(
        old_kernel,
        out_shape=[
            jax.ShapeDtypeStruct((QG, 128), F32),
            jax.ShapeDtypeStruct((QG, 128), F32),
            jax.ShapeDtypeStruct((QG, D), F32),
        ],
        in_specs=[smem_spec(), vmem_spec(), any_spec, any_spec],
        out_specs=[vmem_spec()] * 3,
        scratch_shapes=[
            pltpu.VMEM((HALF, D), BF16),
            pltpu.VMEM((OLD, D, D), BF16),
            pltpu.SemaphoreType.DMA((SLOTS,)),
        ],
        compiler_params=PARAMS,
        name="old",
    )(slot, got, own, label_vectors)
    partner, *state = lax.optimization_barrier((partner, *state))
    leaving = pl.pallas_call(
        score_kernel,
        out_shape=jax.ShapeDtypeStruct((N_CLS, 2, BACK), BF16),
        in_specs=[smem_spec()] * 2 + [vmem_spec(), any_spec] + [vmem_spec()] * 10,
        out_specs=vmem_spec(),
        scratch_shapes=[
            pltpu.VMEM((HALF, D), BF16),
            pltpu.VMEM((QG, D), F32),
            pltpu.SemaphoreType.DMA,
        ],
        compiler_params=PARAMS,
        name="score",
    )(slot, flags, got, own, partner, *state, planes, positive_old, *along_x)
    back = lax.all_to_all(leaving, CLS, 0, 0, tiled=True)
    loss, grads = pl.pallas_call(
        finish_kernel,
        out_shape=[jax.ShapeDtypeStruct((1, 2), F32), jax.ShapeDtypeStruct((1, 2, D), BF16)],
        in_specs=[vmem_spec()] * 2,
        out_specs=[vmem_spec()] * 2,
        compiler_params=PARAMS,
        name="finish",
    )(ids, back)
    return loss, grads, refreshed


def solution(mesh):
    torus = Mesh(
        mesh.devices.reshape(4, 8, 4, mesh.shape["rep"]), ("cls_0", "cls_1", "cls_2", "rep")
    )
    placed = (
        P("rep", CLS, None),
        P(),
        P(CLS, None),
        P(),
        P(CLS_REP, None),
        P(),
        P(),
        P(CLS_REP, None),
        P(),
    )
    return jax.shard_map(
        per_device,
        mesh=torus,
        in_specs=placed,
        out_specs=(P("rep", CLS), P("rep", CLS, None), P(CLS_REP, None)),
        check_vma=False,
    )
```

```python
import jax
import jax.numpy as jnp
from jax import lax
from jax.experimental import pallas as pl
from jax.experimental.pallas import tpu as pltpu
from jax.sharding import Mesh
from jax.sharding import PartitionSpec as P


SLOTS = 8
OLD = SLOTS - 1
D = 768
HALF = 384
QG = 256
N_CLS = 128
PER = 3
CLS = ("cls_0", "cls_1", "cls_2")
CLS_REP = ("cls_0", "cls_1", "cls_2", "rep")
ROWS = PER * HALF
SEND = ROWS + D
QUARTER = 192
BACK = D + 256
F32 = jnp.float32
BF16 = jnp.bfloat16
PARAMS = pltpu.CompilerParams(vmem_limit_bytes=24 * 1024 * 1024)


def vmem_spec():
    return pl.BlockSpec(memory_space=pltpu.VMEM)


def smem_spec():
    return pl.BlockSpec(memory_space=pltpu.SMEM)


def iota(shape, dim):
    return lax.broadcasted_iota(jnp.int32, shape, dim)


def dot(a, b):
    return jnp.dot(a, b, preferred_element_type=F32)


def dot_last(a, b):
    return lax.dot_general(a, b, (((1,), (1,)), ((), ())), preferred_element_type=F32)


def dot_first(a, b):
    return lax.dot_general(a, b, (((0,), (0,)), ((), ())), preferred_element_type=F32)


def one_hot(mask):
    return jnp.where(mask, 1.0, 0.0).astype(BF16)


def spread_down(row):
    return jnp.broadcast_to(row, (128, 128)).T


def own_target_rows():
    row = 3 * lax.axis_index(CLS_REP)
    return row, pl.multiple_of(jnp.minimum(row // 8 * 8, 768 - 16), 8)


def encode_kernel(
    feat_ref, weight_ref, gain_ref, tgt_ref, q_ref, out_ref, row_ref,
    feat_buf, weight_buf, gain_buf, tgt_buf, q_buf, sems,
):
    row, begin = own_target_rows()
    pairs = [
        (tgt_ref.at[pl.ds(begin, 16), :], tgt_buf), (q_ref, q_buf), (weight_ref, weight_buf),
        (feat_ref, feat_buf), (gain_ref, gain_buf),
    ]
    copies = [pltpu.make_async_copy(a, b, sems.at[i]) for i, (a, b) in enumerate(pairs)]
    for copy in copies:
        copy.start()
    copies[0].wait()
    rows = [tgt_buf[pl.ds(row - begin + a, 1), :].astype(F32) for a in range(3)]
    columns = [spread_down(row) for row in rows]
    ranks = []
    for row in rows:
        rank = jnp.zeros((1, 128), F32)
        for column in columns:
            rank += jnp.sum(jnp.where(column < row, 1.0, 0.0), axis=0, keepdims=True)
        ranks.append(rank)
    rank = jnp.concatenate(ranks, axis=1)
    line = iota((QG, HALF), 0)
    first = ((line >> 1) * PER).astype(F32)
    odd = (line & 1) == 1
    chosen = []
    for k in range(PER):
        hit = rank == first + float(k)
        chosen.append((one_hot(hit & ~odd), one_hot(hit & odd)))
    copies[1].wait()
    out_ref[..., ROWS:] = jnp.broadcast_to(q_buf[...], (N_CLS, 2, D))
    for copy in copies[2:]:
        copy.wait()
    hidden = dot(feat_buf[...], weight_buf[...])
    mean = jnp.mean(hidden * hidden, axis=1, keepdims=True)
    gain = jnp.concatenate([gain_buf[i : i + 1, :] for i in range(6)], axis=1)
    encoded = (hidden * lax.rsqrt(mean + 1e-06) * gain).astype(BF16)
    row_ref[...] = encoded
    for k, (even_rows, odd_rows) in enumerate(chosen):
        total = dot(even_rows, encoded[:, :HALF]) + dot(odd_rows, encoded[:, HALF:])
        out_ref[..., k * HALF : (k + 1) * HALF] = total.astype(BF16).reshape(N_CLS, 2, HALF)


def hits_at(plane_ref, label):
    hits = jnp.zeros((QG, 128), F32)
    for k in range(4):
        hits += jnp.where(plane_ref[k] == label, 1.0, 0.0)
    return hits.astype(BF16)


def hits_of(plane_ref, first):
    return hits_at(plane_ref, iota((QG, 128), 1).astype(F32) + first.astype(F32))


def place_kernel(
    slot_ref, tgt_ref, ids_ref, free_ref, row_ref, key_ref, plane_ref, flag_ref, here_ref,
    there_ref, tgt_buf, ids_buf, free_buf, across_ref, sems,
):
    pairs = [(ids_ref, ids_buf), (tgt_ref, tgt_buf), (free_ref, free_buf)]
    copies = [pltpu.make_async_copy(a, b, sems.at[i]) for i, (a, b) in enumerate(pairs)]
    for copy in copies:
        copy.start()
    cls_index, rep_index = lax.axis_index(CLS), lax.axis_index("rep")
    first = cls_index * (SLOTS * D)
    lane = iota((QG, 128), 1)
    seen = jnp.zeros((QG, 128), F32)
    copies[0].wait()

    def plane_of(half, k):
        own = (ids_buf[half, k : k + 1, :] - first).astype(F32)
        return jnp.concatenate([spread_down(own[:, :128]), spread_down(own[:, 128:])], axis=0)

    for k in range(4):
        across_ref[k] = plane_of(1 - rep_index, k)
        plane = plane_of(rep_index, k)
        plane_ref[k] = plane
        seen = jnp.where((plane.astype(jnp.int32) >> 7) == lane, 1.0, seen)
    flag_ref[...] = jnp.max(seen, axis=0, keepdims=True).astype(jnp.int32)

    copies[1].wait()
    base = cls_index * (2 * HALF) + rep_index * HALF
    parts = [tgt_buf[pl.ds(3 * rep_index + a, N_CLS, stride=6), :] for a in range(3)]
    offsets = jnp.concatenate(parts, axis=1) - base
    inside = (offsets >= 0) & (offsets < HALF)
    far = 4096.0
    keys = jnp.where(inside, offsets.astype(F32), far)
    source = iota((N_CLS, QG), 0)
    twice = (iota((N_CLS, QG), 1) >> 1) == source
    for k in range(PER):
        least = jnp.min(keys, axis=1, keepdims=True)
        keys = jnp.where(keys == least, far, keys)
        wide = jnp.broadcast_to(least, (N_CLS, QG))
        key_ref[k : k + 1, :] = jnp.sum(jnp.where(twice, wide, 0.0), axis=0, keepdims=True)

    slot_first = slot_ref[0] * D
    free_first = slot_first + rep_index * HALF
    labels = []
    for part in range(3):
        target = tgt_buf[pl.ds(3 * lax.axis_index(CLS_REP) + part, 1), :]
        owner = ((target >> 8) * 21846) >> 16
        local = (owner - cls_index) * (SLOTS * D) + slot_first + (target - owner * D)
        labels.append(local.astype(F32))
    copies[2].wait()
    for planes, out_ref in ((across_ref, there_ref), (plane_ref, here_ref)):
        total = jnp.zeros((QG, D), F32)
        for part in range(3):
            rows = slice(part * 128, (part + 1) * 128)
            total += dot(hits_of(planes, free_first + part * 128), free_buf[rows, :])
            total += dot(hits_at(planes, labels[part]), row_ref[rows, :])
        out_ref[...] = total.astype(out_ref.dtype)


def positive_kernel(slot_ref, flag_ref, plane_ref, lab_ref, out_ref, lab_buf, sems):
    out_ref[...] = jnp.zeros_like(out_ref)

    def copy_of(i, part):
        tile = (i + (i >= slot_ref[0]).astype(jnp.int32)) * 6 + part
        at = i * 6 + part
        return tile, pltpu.make_async_copy(
            lab_ref.at[pl.ds(tile * 128, 128), :], lab_buf.at[at], sems.at[at]
        )

    for i in range(OLD):
        for part in range(6):
            tile, copy = copy_of(i, part)
            pl.when(flag_ref[0, tile] > 0)(copy.start)

    def body(at, carry):
        i = at // 6
        tile, copy = copy_of(i, at - i * 6)

        @pl.when(flag_ref[0, tile] > 0)
        def _():
            copy.wait()
            out_ref[...] += dot(hits_of(plane_ref, tile * 128), lab_buf[at])

        return carry

    lax.fori_loop(0, OLD * 6, body, 0)


def quarter_kernel(old_ref, here_ref, came_ref, *out_refs):
    total = (old_ref[...] + here_ref[...] + came_ref[...].astype(F32)).astype(BF16)
    line, lane = iota((D, 256), 0), iota((D, 256), 1)
    for shift, out_ref in enumerate(out_refs):
        first = ((lax.axis_index("cls_2") + shift) & 3) * QUARTER
        pick = one_hot((line == first + lane) & (lane < QUARTER))
        out_ref[...] = dot(total, pick).astype(BF16)


def refresh_kernel(key_ref, got_ref, free_ref, *refs):
    out_ref = refs[-1]
    own = iota((HALF, QG), 0).astype(F32)
    odd = (iota((HALF, QG), 1) & 1) == 1
    matches = [key_ref[k : k + 1, :] == own for k in range(PER)]
    got = [got_ref[..., k * HALF : (k + 1) * HALF].reshape(QG, HALF) for k in range(PER)]
    for h in range(2):
        cols = slice(h * HALF, (h + 1) * HALF)
        mine = odd if h else ~odd
        placed = jnp.zeros((HALF, HALF), F32)
        for k in range(PER):
            placed += dot(one_hot(matches[k] & mine), got[k])
        out_ref[:, cols] = (free_ref[:, cols].astype(F32) + placed).astype(BF16)


def three_parts(value):
    high = value.astype(BF16).astype(F32)
    rest = value - high
    middle = rest.astype(BF16).astype(F32)
    return [high, middle, rest - middle]


def over_lanes(fn, value):
    total = value[:, :128]
    for at in range(128, value.shape[1], 128):
        total = fn(total, value[:, at : at + 128])
    return total


def absorb_all(state, queries, blocks, waits):
    peak, total, grads = state

    def logits_of(i):
        for copy in waits[i]:
            copy.wait()
        return dot_last(queries, blocks[i][...])

    following = logits_of(0)
    for i, block in enumerate(blocks):
        logits = following
        if i + 1 < len(blocks):
            following = logits_of(i + 1)
        higher = jnp.maximum(peak, jnp.max(over_lanes(jnp.maximum, logits), axis=1, keepdims=True))
        scale = jnp.exp(peak - higher)
        weight = jnp.exp(logits - higher)
        total = total * scale + over_lanes(jnp.add, weight)
        grads = grads * scale + dot(weight.astype(BF16), block[...])
        peak = higher
    return peak, total, grads


def old_kernel(
    slot_ref, got_ref, own_ref, lab_ref, peak_ref, total_ref, grad_ref, own_buf, lab_buf, sems
):
    slot = slot_ref[0]
    own_copy = pltpu.make_async_copy(own_ref, own_buf, sems.at[OLD])
    own_copy.start()
    copies = []
    for i in range(OLD):
        source = (i + (i >= slot).astype(jnp.int32)) * D
        copies.append(
            pltpu.make_async_copy(lab_ref.at[pl.ds(source, D), :], lab_buf.at[i], sems.at[i])
        )
        copies[-1].start()
    start = (jnp.full((QG, 1), -jnp.inf, F32), jnp.zeros((QG, 128), F32), jnp.zeros((QG, D), F32))
    peak, total, grads = absorb_all(
        start,
        got_ref[..., ROWS:].reshape(QG, D),
        [own_buf] + [lab_buf.at[i] for i in range(OLD)],
        [[own_copy]] + [[copy] for copy in copies],
    )
    peak_ref[...] = jnp.broadcast_to(peak, (QG, 128))
    total_ref[...] = total
    grad_ref[...] = grads


def score_kernel(
    slot_ref, flag_ref, got_ref, own_ref, other_ref, peak_ref, total_ref, grad_ref, plane_ref,
    pos_ref, *refs
):
    quarter_refs, (out_ref, own_buf, pos_buf, sem) = refs[:4], refs[4:]
    rep = lax.axis_index("rep")
    slot = slot_ref[0]
    own_copy = pltpu.make_async_copy(own_ref, own_buf, sem)
    own_copy.start()
    queries = got_ref[..., ROWS:].reshape(QG, D)
    state = (peak_ref[:, :1], total_ref[...], grad_ref[...])
    peak, total, grads = absorb_all(state, queries, [other_ref], [[]])
    out_ref[..., :D] = grads.astype(BF16).reshape(N_CLS, 2, D)
    pos_buf[...] = pos_ref[...]
    own_copy.wait()
    for block, half in ((own_buf, rep), (other_ref, 1 - rep)):
        for part in range(3):
            tile = slot * 6 + half * 3 + part

            @pl.when(flag_ref[0, tile] > 0)
            def _():
                rows = block[part * 128 : (part + 1) * 128, :]
                pos_buf[...] += dot(hits_of(plane_ref, tile * 128), rows)

    positive = pos_buf[...]
    picked = jnp.sum(queries.astype(F32) * positive, axis=1, keepdims=True)
    exp_total = jnp.sum(total, axis=1, keepdims=True)
    lane = iota((QG, 256), 1)
    tail = sum(ref[...].astype(F32) for ref in quarter_refs)
    for at, part in enumerate(three_parts(peak) + three_parts(exp_total) + three_parts(picked)):
        tail = jnp.where(lane == QUARTER + at, part, tail)
    out_ref[..., D:] = tail.astype(BF16).reshape(N_CLS, 2, 256)


def finish_kernel(ids_ref, back_ref, loss_ref, grad_ref):
    back = back_ref[...].reshape(QG, BACK)
    tail = back[:, D:].astype(F32)
    stats = tail[:, 128:]

    def column(at):
        at += QUARTER - 128
        return stats[:, at : at + 1] + stats[:, at + 1 : at + 2] + stats[:, at + 2 : at + 3]

    peak, total, picked = column(0), column(3), column(6)
    odd = (iota((QG, 1), 0) & 1) == 1
    ring = (iota((QG, 1), 0) >> 1) & 3
    valid = jnp.where(ids_ref[lax.axis_index("rep")] >= 0, 1.0, 0.0)
    column_of = iota((4, QG), 1) - 2 * lax.axis_index(CLS)
    losses, weights, picks = [], [], []
    for h in range(2):
        mine = odd if h else ~odd
        top = jnp.max(jnp.where(mine, peak, -jnp.inf), axis=0, keepdims=True)
        weight = jnp.where(mine, jnp.exp(peak - top), 0.0)
        exp_total = jnp.sum(weight * total, axis=0, keepdims=True)
        count = jnp.sum(jnp.where(column_of == h, valid, 0.0), axis=1, keepdims=True)
        inverse = 1.0 / jnp.sum(count, axis=0, keepdims=True)
        chosen = jnp.sum(jnp.where(mine, picked, 0.0), axis=0, keepdims=True)
        losses.append(top + jnp.log(exp_total) - chosen * inverse)
        weights.append(weight / exp_total)
        picks.append(inverse)
    loss_ref[...] = jnp.concatenate(losses, axis=1)
    lane = iota((QG, 128), 1)
    table = jnp.where(lane == 8 + 4 * jnp.where(odd, 1, 0) + ring, 1.0, 0.0)
    for h in range(2):
        for at, part in enumerate(three_parts(weights[h])):
            table = jnp.where(lane == 3 * h + at, part, table)
    sums = dot_first(table.astype(BF16), back)
    grads = []
    for h in range(2):
        positive = jnp.concatenate(
            [sums[8 + 4 * h + x : 9 + 4 * h + x, D : D + QUARTER] for x in range(4)], axis=1
        )
        scaled = sums[3 * h : 3 * h + 1, :D] + sums[3 * h + 1 : 3 * h + 2, :D]
        scaled += sums[3 * h + 2 : 3 * h + 3, :D]
        grads.append(scaled - positive * picks[h])
    grad_ref[...] = jnp.concatenate(grads, axis=0).astype(BF16).reshape(1, 2, D)


def in_hbm(value):
    return pltpu.with_memory_space_constraint(value, pltpu.HBM)


def per_device(
    queries,
    positives,
    label_vectors,
    refresh_slot,
    features,
    encoder_weight,
    encoder_gain,
    free_vectors,
    targets,
):
    target_rows = targets.reshape(768, 128)
    label_vectors = in_hbm(label_vectors)
    slot = refresh_slot.reshape(1)
    ids = positives.transpose(0, 2, 1)

    any_spec = pl.BlockSpec(memory_space=pl.ANY)
    sending, encoded = pl.pallas_call(
        encode_kernel,
        out_shape=[
            jax.ShapeDtypeStruct((N_CLS, 2, SEND), BF16),
            jax.ShapeDtypeStruct((HALF, D), BF16),
        ],
        in_specs=[any_spec] * 5,
        out_specs=[vmem_spec()] * 2,
        scratch_shapes=[
            pltpu.VMEM((HALF, D), BF16),
            pltpu.VMEM((D, D), BF16),
            pltpu.VMEM((6, 128), F32),
            pltpu.VMEM((16, 128), jnp.int32),
            pltpu.VMEM((1, 2, D), BF16),
            pltpu.SemaphoreType.DMA((5,)),
        ],
        compiler_params=PARAMS,
        name="encode",
    )(
        in_hbm(features),
        in_hbm(encoder_weight),
        in_hbm(encoder_gain.reshape(6, 128)),
        in_hbm(target_rows),
        in_hbm(queries),
    )
    keys, planes, flags, here, there = pl.pallas_call(
        place_kernel,
        out_shape=[
            jax.ShapeDtypeStruct((8, QG), F32),
            jax.ShapeDtypeStruct((4, QG, 128), F32),
            jax.ShapeDtypeStruct((1, 128), jnp.int32),
            jax.ShapeDtypeStruct((QG, D), F32),
            jax.ShapeDtypeStruct((QG, D), BF16),
        ],
        in_specs=[smem_spec()] + [any_spec] * 3 + [vmem_spec()],
        out_specs=[vmem_spec()] * 5,
        scratch_shapes=[
            pltpu.VMEM((768, 128), jnp.int32),
            pltpu.VMEM((2, 4, QG), jnp.int32),
            pltpu.VMEM((HALF, D), BF16),
            pltpu.VMEM((4, QG, 128), F32),
            pltpu.SemaphoreType.DMA((3,)),
        ],
        compiler_params=PARAMS,
        name="place",
    )(slot, in_hbm(target_rows), in_hbm(ids), in_hbm(free_vectors), encoded)
    got = lax.all_to_all(sending, CLS, 0, 0, tiled=True)

    positive_old = pl.pallas_call(
        positive_kernel,
        out_shape=jax.ShapeDtypeStruct((QG, D), F32),
        in_specs=[smem_spec()] * 2 + [vmem_spec(), any_spec],
        out_specs=vmem_spec(),
        scratch_shapes=[
            pltpu.VMEM((OLD * 6, 128, D), BF16),
            pltpu.SemaphoreType.DMA((OLD * 6,)),
        ],
        compiler_params=PARAMS,
        name="positive",
    )(slot, flags, planes, label_vectors)

    came = lax.ppermute(there, "rep", [(0, 1), (1, 0)])
    quarters = pl.pallas_call(
        quarter_kernel,
        out_shape=[jax.ShapeDtypeStruct((QG, 256), BF16)] * 4,
        in_specs=[vmem_spec()] * 3,
        out_specs=[vmem_spec()] * 4,
        compiler_params=PARAMS,
        name="quarter",
    )(positive_old, here, came)
    along_x = [quarters[0]]
    for shift in (1, 2, 3):
        pairs = [(x, (x + shift) % 4) for x in range(4)]
        along_x.append(lax.ppermute(quarters[shift], "cls_2", pairs))

    refreshed = pl.pallas_call(
        refresh_kernel,
        out_shape=jax.ShapeDtypeStruct((HALF, D), BF16),
        in_specs=[vmem_spec()] * 3 + [any_spec],
        out_specs=vmem_spec(),
        compiler_params=PARAMS,
        name="refresh",
    )(keys, got, free_vectors, quarters[0])
    partner = lax.ppermute(refreshed, "rep", [(0, 1), (1, 0)])

    own = in_hbm(refreshed)
    state = pl.pallas_call(
        old_kernel,
        out_shape=[
            jax.ShapeDtypeStruct((QG, 128), F32),
            jax.ShapeDtypeStruct((QG, 128), F32),
            jax.ShapeDtypeStruct((QG, D), F32),
        ],
        in_specs=[smem_spec(), vmem_spec(), any_spec, any_spec],
        out_specs=[vmem_spec()] * 3,
        scratch_shapes=[
            pltpu.VMEM((HALF, D), BF16),
            pltpu.VMEM((OLD, D, D), BF16),
            pltpu.SemaphoreType.DMA((SLOTS,)),
        ],
        compiler_params=PARAMS,
        name="old",
    )(slot, got, own, label_vectors)
    partner, *state = lax.optimization_barrier((partner, *state))
    leaving = pl.pallas_call(
        score_kernel,
        out_shape=jax.ShapeDtypeStruct((N_CLS, 2, BACK), BF16),
        in_specs=[smem_spec()] * 2 + [vmem_spec(), any_spec] + [vmem_spec()] * 10,
        out_specs=vmem_spec(),
        scratch_shapes=[
            pltpu.VMEM((HALF, D), BF16),
            pltpu.VMEM((QG, D), F32),
            pltpu.SemaphoreType.DMA,
        ],
        compiler_params=PARAMS,
        name="score",
    )(slot, flags, got, own, partner, *state, planes, positive_old, *along_x)
    back = lax.all_to_all(leaving, CLS, 0, 0, tiled=True)
    loss, grads = pl.pallas_call(
        finish_kernel,
        out_shape=[jax.ShapeDtypeStruct((1, 2), F32), jax.ShapeDtypeStruct((1, 2, D), BF16)],
        in_specs=[vmem_spec()] * 2,
        out_specs=[vmem_spec()] * 2,
        compiler_params=PARAMS,
        name="finish",
    )(ids, back)
    return loss, grads, refreshed


def solution(mesh):
    torus = Mesh(
        mesh.devices.reshape(4, 8, 4, mesh.shape["rep"]), ("cls_0", "cls_1", "cls_2", "rep")
    )
    placed = (
        P("rep", CLS, None),
        P(),
        P(CLS, None),
        P(),
        P(CLS_REP, None),
        P(),
        P(),
        P(CLS_REP, None),
        P(),
    )
    return jax.shard_map(
        per_device,
        mesh=torus,
        in_specs=placed,
        out_specs=(P("rep", CLS), P("rep", CLS, None), P(CLS_REP, None)),
        check_vma=False,
    )
```

```python
import jax
import jax.numpy as jnp
from jax import lax
from jax.experimental import pallas as pl
from jax.experimental.pallas import tpu as pltpu
from jax.sharding import Mesh
from jax.sharding import PartitionSpec as P


SLOTS = 8
OLD = SLOTS - 1
D = 768
HALF = 384
QG = 256
N_CLS = 128
PER = 3
CLS = ("cls_0", "cls_1", "cls_2")
CLS_REP = ("cls_0", "cls_1", "cls_2", "rep")
ROWS = PER * HALF
SEND = ROWS + D
QUARTER = 192
BACK = D + 256
F32 = jnp.float32
BF16 = jnp.bfloat16
PARAMS = pltpu.CompilerParams(vmem_limit_bytes=24 * 1024 * 1024)


def vmem_spec():
    return pl.BlockSpec(memory_space=pltpu.VMEM)


def smem_spec():
    return pl.BlockSpec(memory_space=pltpu.SMEM)


def iota(shape, dim):
    return lax.broadcasted_iota(jnp.int32, shape, dim)


def dot(a, b):
    return jnp.dot(a, b, preferred_element_type=F32)


def dot_last(a, b):
    return lax.dot_general(a, b, (((1,), (1,)), ((), ())), preferred_element_type=F32)


def dot_first(a, b):
    return lax.dot_general(a, b, (((0,), (0,)), ((), ())), preferred_element_type=F32)


def one_hot(mask):
    return jnp.where(mask, 1.0, 0.0).astype(BF16)


def spread_down(row):
    return jnp.broadcast_to(row, (128, 128)).T


def own_target_rows():
    row = 3 * lax.axis_index(CLS_REP)
    return row, pl.multiple_of(jnp.minimum(row // 8 * 8, 768 - 16), 8)


def encode_kernel(
    feat_ref, weight_ref, gain_ref, tgt_ref, q_ref, out_ref, row_ref,
    feat_buf, weight_buf, gain_buf, tgt_buf, q_buf, out_buf, sems,
):
    row, begin = own_target_rows()
    pairs = [
        (tgt_ref.at[pl.ds(begin, 16), :], tgt_buf), (q_ref, q_buf), (feat_ref, feat_buf),
        (weight_ref.at[pl.ds(0, HALF), :], weight_buf.at[pl.ds(0, HALF), :]),
        (weight_ref.at[pl.ds(HALF, HALF), :], weight_buf.at[pl.ds(HALF, HALF), :]),
        (gain_ref, gain_buf),
    ]
    copies = [pltpu.make_async_copy(a, b, sems.at[i]) for i, (a, b) in enumerate(pairs)]
    for copy in copies:
        copy.start()
    copies[0].wait()
    rows = [tgt_buf[pl.ds(row - begin + a, 1), :].astype(F32) for a in range(3)]
    columns = [spread_down(row) for row in rows]
    ranks = []
    for row in rows:
        rank = jnp.zeros((1, 128), F32)
        for column in columns:
            rank += jnp.sum(jnp.where(column < row, 1.0, 0.0), axis=0, keepdims=True)
        ranks.append(rank)
    rank = jnp.concatenate(ranks, axis=1)
    line = iota((QG, HALF), 0)
    first = ((line >> 1) * PER).astype(F32)
    odd = (line & 1) == 1
    chosen = []
    for k in range(PER):
        hit = rank == first + float(k)
        chosen.append((one_hot(hit & ~odd), one_hot(hit & odd)))
    copies[1].wait()
    leaving = []

    def send(first, value):
        window = pl.ds(first, value.shape[2])
        out_buf[:, :, first : first + value.shape[2]] = value
        at = 6 + len(leaving)
        copy = pltpu.make_async_copy(
            out_buf.at[:, :, window], out_ref.at[:, :, window], sems.at[at]
        )
        copy.start()
        leaving.append(copy)

    send(ROWS, jnp.broadcast_to(q_buf[...], (N_CLS, 2, D)))
    copies[2].wait()
    copies[3].wait()
    hidden = dot(feat_buf[:, :HALF], weight_buf[:HALF, :])
    copies[4].wait()
    hidden += dot(feat_buf[:, HALF:], weight_buf[HALF:, :])
    copies[5].wait()
    mean = jnp.mean(hidden * hidden, axis=1, keepdims=True)
    gain = jnp.concatenate([gain_buf[i : i + 1, :] for i in range(6)], axis=1)
    encoded = (hidden * lax.rsqrt(mean + 1e-06) * gain).astype(BF16)
    row_ref[...] = encoded
    for k, (even_rows, odd_rows) in enumerate(chosen):
        total = dot(even_rows, encoded[:, :HALF]) + dot(odd_rows, encoded[:, HALF:])
        send(k * HALF, total.astype(BF16).reshape(N_CLS, 2, HALF))
    for copy in leaving:
        copy.wait()


def hits_at(plane_ref, label):
    hits = jnp.zeros((QG, 128), F32)
    for k in range(4):
        hits += jnp.where(plane_ref[k] == label, 1.0, 0.0)
    return hits.astype(BF16)


def hits_of(plane_ref, first):
    return hits_at(plane_ref, iota((QG, 128), 1).astype(F32) + first.astype(F32))


def place_kernel(
    slot_ref, tgt_ref, ids_ref, free_ref, row_ref, key_ref, plane_ref, flag_ref, here_ref,
    there_ref, tgt_buf, ids_buf, free_buf, across_ref, sems,
):
    pairs = [(ids_ref, ids_buf), (tgt_ref, tgt_buf), (free_ref, free_buf)]
    copies = [pltpu.make_async_copy(a, b, sems.at[i]) for i, (a, b) in enumerate(pairs)]
    for copy in copies:
        copy.start()
    cls_index, rep_index = lax.axis_index(CLS), lax.axis_index("rep")
    first = cls_index * (SLOTS * D)
    lane = iota((QG, 128), 1)
    seen = jnp.zeros((QG, 128), F32)
    copies[0].wait()

    def plane_of(half, k):
        own = (ids_buf[half, k : k + 1, :] - first).astype(F32)
        return jnp.concatenate([spread_down(own[:, :128]), spread_down(own[:, 128:])], axis=0)

    for k in range(4):
        across_ref[k] = plane_of(1 - rep_index, k)
        plane = plane_of(rep_index, k)
        plane_ref[k] = plane
        seen = jnp.where((plane.astype(jnp.int32) >> 7) == lane, 1.0, seen)
    flag_ref[...] = jnp.max(seen, axis=0, keepdims=True).astype(jnp.int32)

    copies[1].wait()
    base = cls_index * (2 * HALF) + rep_index * HALF
    parts = [tgt_buf[pl.ds(3 * rep_index + a, N_CLS, stride=6), :] for a in range(3)]
    offsets = jnp.concatenate(parts, axis=1) - base
    inside = (offsets >= 0) & (offsets < HALF)
    far = 4096.0
    keys = jnp.where(inside, offsets.astype(F32), far)
    source = iota((N_CLS, QG), 0)
    twice = (iota((N_CLS, QG), 1) >> 1) == source
    for k in range(PER):
        least = jnp.min(keys, axis=1, keepdims=True)
        keys = jnp.where(keys == least, far, keys)
        wide = jnp.broadcast_to(least, (N_CLS, QG))
        key_ref[k : k + 1, :] = jnp.sum(jnp.where(twice, wide, 0.0), axis=0, keepdims=True)

    slot_first = slot_ref[0] * D
    free_first = slot_first + rep_index * HALF
    labels = []
    for part in range(3):
        target = tgt_buf[pl.ds(3 * lax.axis_index(CLS_REP) + part, 1), :]
        owner = ((target >> 8) * 21846) >> 16
        local = (owner - cls_index) * (SLOTS * D) + slot_first + (target - owner * D)
        labels.append(local.astype(F32))
    copies[2].wait()
    for planes, out_ref in ((across_ref, there_ref), (plane_ref, here_ref)):
        total = jnp.zeros((QG, D), F32)
        for part in range(3):
            rows = slice(part * 128, (part + 1) * 128)
            total += dot(hits_of(planes, free_first + part * 128), free_buf[rows, :])
            total += dot(hits_at(planes, labels[part]), row_ref[rows, :])
        out_ref[...] = total.astype(out_ref.dtype)


def positive_kernel(slot_ref, flag_ref, plane_ref, lab_ref, out_ref, lab_buf, sems):
    out_ref[...] = jnp.zeros_like(out_ref)

    def copy_of(i, part):
        tile = (i + (i >= slot_ref[0]).astype(jnp.int32)) * 6 + part
        at = i * 6 + part
        return tile, pltpu.make_async_copy(
            lab_ref.at[pl.ds(tile * 128, 128), :], lab_buf.at[at], sems.at[at]
        )

    for i in range(OLD):
        for part in range(6):
            tile, copy = copy_of(i, part)
            pl.when(flag_ref[0, tile] > 0)(copy.start)

    def body(at, carry):
        i = at // 6
        tile, copy = copy_of(i, at - i * 6)

        @pl.when(flag_ref[0, tile] > 0)
        def _():
            copy.wait()
            out_ref[...] += dot(hits_of(plane_ref, tile * 128), lab_buf[at])

        return carry

    lax.fori_loop(0, OLD * 6, body, 0)


def quarter_kernel(old_ref, here_ref, came_ref, *out_refs):
    total = (old_ref[...] + here_ref[...] + came_ref[...].astype(F32)).astype(BF16)
    line, lane = iota((D, 256), 0), iota((D, 256), 1)
    for shift, out_ref in enumerate(out_refs):
        first = ((lax.axis_index("cls_2") + shift) & 3) * QUARTER
        pick = one_hot((line == first + lane) & (lane < QUARTER))
        out_ref[...] = dot(total, pick).astype(BF16)


def refresh_kernel(key_ref, got_ref, free_ref, *refs):
    out_ref = refs[-1]
    own = iota((HALF, QG), 0).astype(F32)
    odd = (iota((HALF, QG), 1) & 1) == 1
    matches = [key_ref[k : k + 1, :] == own for k in range(PER)]
    got = [got_ref[..., k * HALF : (k + 1) * HALF].reshape(QG, HALF) for k in range(PER)]
    for h in range(2):
        cols = slice(h * HALF, (h + 1) * HALF)
        mine = odd if h else ~odd
        placed = jnp.zeros((HALF, HALF), F32)
        for k in range(PER):
            placed += dot(one_hot(matches[k] & mine), got[k])
        out_ref[:, cols] = (free_ref[:, cols].astype(F32) + placed).astype(BF16)


def three_parts(value):
    high = value.astype(BF16).astype(F32)
    rest = value - high
    middle = rest.astype(BF16).astype(F32)
    return [high, middle, rest - middle]


def over_lanes(fn, value):
    total = value[:, :128]
    for at in range(128, value.shape[1], 128):
        total = fn(total, value[:, at : at + 128])
    return total


def absorb_all(state, queries, blocks, waits):
    peak, total, grads = state

    def logits_of(i):
        for copy in waits[i]:
            copy.wait()
        return dot_last(queries, blocks[i][...])

    following = logits_of(0)
    for i, block in enumerate(blocks):
        logits = following
        if i + 1 < len(blocks):
            following = logits_of(i + 1)
        higher = jnp.maximum(peak, jnp.max(over_lanes(jnp.maximum, logits), axis=1, keepdims=True))
        scale = jnp.exp(peak - higher)
        weight = jnp.exp(logits - higher)
        total = total * scale + over_lanes(jnp.add, weight)
        grads = grads * scale + dot(weight.astype(BF16), block[...])
        peak = higher
    return peak, total, grads


def old_kernel(
    slot_ref, got_ref, own_ref, lab_ref, out_ref, peak_ref, total_ref, grad_ref, lab_buf, sems
):
    slot = slot_ref[0]
    copies = []
    for i in range(OLD):
        source = (i + (i >= slot).astype(jnp.int32)) * D
        copies.append(
            pltpu.make_async_copy(lab_ref.at[pl.ds(source, D), :], lab_buf.at[i], sems.at[i])
        )
        copies[-1].start()
    out_copy = pltpu.make_async_copy(own_ref, out_ref, sems.at[OLD])
    out_copy.start()
    start = (jnp.full((QG, 1), -jnp.inf, F32), jnp.zeros((QG, 128), F32), jnp.zeros((QG, D), F32))
    peak, total, grads = absorb_all(
        start,
        got_ref[..., ROWS:].reshape(QG, D),
        [own_ref] + [lab_buf.at[i] for i in range(OLD)],
        [[]] + [[copy] for copy in copies],
    )
    peak_ref[...] = jnp.broadcast_to(peak, (QG, 128))
    total_ref[...] = total
    grad_ref[...] = grads
    out_copy.wait()


def score_kernel(
    slot_ref, flag_ref, got_ref, own_ref, other_ref, peak_ref, total_ref, grad_ref, plane_ref,
    pos_ref, *refs
):
    quarter_refs, (out_ref, pos_buf) = refs[:4], refs[4:]
    rep = lax.axis_index("rep")
    slot = slot_ref[0]
    queries = got_ref[..., ROWS:].reshape(QG, D)
    state = (peak_ref[:, :1], total_ref[...], grad_ref[...])
    peak, total, grads = absorb_all(state, queries, [other_ref], [[]])
    out_ref[..., :D] = grads.astype(BF16).reshape(N_CLS, 2, D)
    pos_buf[...] = pos_ref[...]
    for block, half in ((own_ref, rep), (other_ref, 1 - rep)):
        for part in range(3):
            tile = slot * 6 + half * 3 + part

            @pl.when(flag_ref[0, tile] > 0)
            def _():
                rows = block[part * 128 : (part + 1) * 128, :]
                pos_buf[...] += dot(hits_of(plane_ref, tile * 128), rows)

    positive = pos_buf[...]
    picked = jnp.sum(queries.astype(F32) * positive, axis=1, keepdims=True)
    exp_total = jnp.sum(total, axis=1, keepdims=True)
    lane = iota((QG, 256), 1)
    tail = sum(ref[...].astype(F32) for ref in quarter_refs)
    for at, part in enumerate(three_parts(peak) + three_parts(exp_total) + three_parts(picked)):
        tail = jnp.where(lane == QUARTER + at, part, tail)
    out_ref[..., D:] = tail.astype(BF16).reshape(N_CLS, 2, 256)


def finish_kernel(ids_ref, back_ref, loss_ref, grad_ref):
    back = back_ref[...].reshape(QG, BACK)
    tail = back[:, D:].astype(F32)
    stats = tail[:, 128:]

    def column(at):
        at += QUARTER - 128
        return stats[:, at : at + 1] + stats[:, at + 1 : at + 2] + stats[:, at + 2 : at + 3]

    peak, total, picked = column(0), column(3), column(6)
    odd = (iota((QG, 1), 0) & 1) == 1
    ring = (iota((QG, 1), 0) >> 1) & 3
    valid = jnp.where(ids_ref[lax.axis_index("rep")] >= 0, 1.0, 0.0)
    column_of = iota((4, QG), 1) - 2 * lax.axis_index(CLS)
    losses, weights, picks = [], [], []
    for h in range(2):
        mine = odd if h else ~odd
        top = jnp.max(jnp.where(mine, peak, -jnp.inf), axis=0, keepdims=True)
        weight = jnp.where(mine, jnp.exp(peak - top), 0.0)
        exp_total = jnp.sum(weight * total, axis=0, keepdims=True)
        count = jnp.sum(jnp.where(column_of == h, valid, 0.0), axis=1, keepdims=True)
        inverse = 1.0 / jnp.sum(count, axis=0, keepdims=True)
        chosen = jnp.sum(jnp.where(mine, picked, 0.0), axis=0, keepdims=True)
        losses.append(top + jnp.log(exp_total) - chosen * inverse)
        weights.append(weight / exp_total)
        picks.append(inverse)
    loss_ref[...] = jnp.concatenate(losses, axis=1)
    lane = iota((QG, 128), 1)
    table = jnp.where(lane == 8 + 4 * jnp.where(odd, 1, 0) + ring, 1.0, 0.0)
    for h in range(2):
        for at, part in enumerate(three_parts(weights[h])):
            table = jnp.where(lane == 3 * h + at, part, table)
    sums = dot_first(table.astype(BF16), back)
    grads = []
    for h in range(2):
        positive = jnp.concatenate(
            [sums[8 + 4 * h + x : 9 + 4 * h + x, D : D + QUARTER] for x in range(4)], axis=1
        )
        scaled = sums[3 * h : 3 * h + 1, :D] + sums[3 * h + 1 : 3 * h + 2, :D]
        scaled += sums[3 * h + 2 : 3 * h + 3, :D]
        grads.append(scaled - positive * picks[h])
    grad_ref[...] = jnp.concatenate(grads, axis=0).astype(BF16).reshape(1, 2, D)


def in_hbm(value):
    return pltpu.with_memory_space_constraint(value, pltpu.HBM)


def per_device(
    queries,
    positives,
    label_vectors,
    refresh_slot,
    features,
    encoder_weight,
    encoder_gain,
    free_vectors,
    targets,
):
    target_rows = targets.reshape(768, 128)
    label_vectors = in_hbm(label_vectors)
    slot = refresh_slot.reshape(1)
    ids = positives.transpose(0, 2, 1)

    any_spec = pl.BlockSpec(memory_space=pl.ANY)
    sending, encoded = pl.pallas_call(
        encode_kernel,
        out_shape=[
            pltpu.HBM((N_CLS, 2, SEND), BF16),
            jax.ShapeDtypeStruct((HALF, D), BF16),
        ],
        in_specs=[any_spec] * 5,
        out_specs=[any_spec, vmem_spec()],
        scratch_shapes=[
            pltpu.VMEM((HALF, D), BF16),
            pltpu.VMEM((D, D), BF16),
            pltpu.VMEM((6, 128), F32),
            pltpu.VMEM((16, 128), jnp.int32),
            pltpu.VMEM((1, 2, D), BF16),
            pltpu.VMEM((N_CLS, 2, SEND), BF16),
            pltpu.SemaphoreType.DMA((10,)),
        ],
        compiler_params=PARAMS,
        name="encode",
    )(
        in_hbm(features),
        in_hbm(encoder_weight),
        in_hbm(encoder_gain.reshape(6, 128)),
        in_hbm(target_rows),
        in_hbm(queries),
    )
    keys, planes, flags, here, there = pl.pallas_call(
        place_kernel,
        out_shape=[
            jax.ShapeDtypeStruct((8, QG), F32),
            jax.ShapeDtypeStruct((4, QG, 128), F32),
            jax.ShapeDtypeStruct((1, 128), jnp.int32),
            jax.ShapeDtypeStruct((QG, D), F32),
            jax.ShapeDtypeStruct((QG, D), BF16),
        ],
        in_specs=[smem_spec()] + [any_spec] * 3 + [vmem_spec()],
        out_specs=[vmem_spec()] * 5,
        scratch_shapes=[
            pltpu.VMEM((768, 128), jnp.int32),
            pltpu.VMEM((2, 4, QG), jnp.int32),
            pltpu.VMEM((HALF, D), BF16),
            pltpu.VMEM((4, QG, 128), F32),
            pltpu.SemaphoreType.DMA((3,)),
        ],
        compiler_params=PARAMS,
        name="place",
    )(slot, in_hbm(target_rows), in_hbm(ids), in_hbm(free_vectors), encoded)
    got = lax.all_to_all(sending, CLS, 0, 0, tiled=True)

    positive_old = pl.pallas_call(
        positive_kernel,
        out_shape=jax.ShapeDtypeStruct((QG, D), F32),
        in_specs=[smem_spec()] * 2 + [vmem_spec(), any_spec],
        out_specs=vmem_spec(),
        scratch_shapes=[
            pltpu.VMEM((OLD * 6, 128, D), BF16),
            pltpu.SemaphoreType.DMA((OLD * 6,)),
        ],
        compiler_params=PARAMS,
        name="positive",
    )(slot, flags, planes, label_vectors)

    came = lax.ppermute(there, "rep", [(0, 1), (1, 0)])
    quarters = pl.pallas_call(
        quarter_kernel,
        out_shape=[jax.ShapeDtypeStruct((QG, 256), BF16)] * 4,
        in_specs=[vmem_spec()] * 3,
        out_specs=[vmem_spec()] * 4,
        compiler_params=PARAMS,
        name="quarter",
    )(positive_old, here, came)
    along_x = [quarters[0]]
    for shift in (1, 2, 3):
        pairs = [(x, (x + shift) % 4) for x in range(4)]
        along_x.append(lax.ppermute(quarters[shift], "cls_2", pairs))

    own = pl.pallas_call(
        refresh_kernel,
        out_shape=jax.ShapeDtypeStruct((HALF, D), BF16),
        in_specs=[vmem_spec()] * 3 + [any_spec],
        out_specs=vmem_spec(),
        compiler_params=PARAMS,
        name="refresh",
    )(keys, got, free_vectors, quarters[0])
    partner = lax.ppermute(own, "rep", [(0, 1), (1, 0)])

    refreshed, *state = pl.pallas_call(
        old_kernel,
        out_shape=[
            pltpu.HBM((HALF, D), BF16),
            jax.ShapeDtypeStruct((QG, 128), F32),
            jax.ShapeDtypeStruct((QG, 128), F32),
            jax.ShapeDtypeStruct((QG, D), F32),
        ],
        in_specs=[smem_spec(), vmem_spec(), vmem_spec(), any_spec],
        out_specs=[any_spec] + [vmem_spec()] * 3,
        scratch_shapes=[
            pltpu.VMEM((OLD, D, D), BF16),
            pltpu.SemaphoreType.DMA((SLOTS,)),
        ],
        compiler_params=PARAMS,
        name="old",
    )(slot, got, own, label_vectors)
    partner, *state = lax.optimization_barrier((partner, *state))
    leaving = pl.pallas_call(
        score_kernel,
        out_shape=jax.ShapeDtypeStruct((N_CLS, 2, BACK), BF16),
        in_specs=[smem_spec()] * 2 + [vmem_spec()] * 12,
        out_specs=vmem_spec(),
        scratch_shapes=[
            pltpu.VMEM((QG, D), F32),
        ],
        compiler_params=PARAMS,
        name="score",
    )(slot, flags, got, own, partner, *state, planes, positive_old, *along_x)
    back = lax.all_to_all(leaving, CLS, 0, 0, tiled=True)
    loss, grads = pl.pallas_call(
        finish_kernel,
        out_shape=[jax.ShapeDtypeStruct((1, 2), F32), jax.ShapeDtypeStruct((1, 2, D), BF16)],
        in_specs=[vmem_spec()] * 2,
        out_specs=[vmem_spec()] * 2,
        compiler_params=PARAMS,
        name="finish",
    )(ids, back)
    return loss, grads, refreshed


def solution(mesh):
    torus = Mesh(
        mesh.devices.reshape(4, 8, 4, mesh.shape["rep"]), ("cls_0", "cls_1", "cls_2", "rep")
    )
    placed = (
        P("rep", CLS, None),
        P(),
        P(CLS, None),
        P(),
        P(CLS_REP, None),
        P(),
        P(),
        P(CLS_REP, None),
        P(),
    )
    return jax.shard_map(
        per_device,
        mesh=torus,
        in_specs=placed,
        out_specs=(P("rep", CLS), P("rep", CLS, None), P(CLS_REP, None)),
        check_vma=False,
    )
```

```python
import jax
import jax.numpy as jnp
from jax import lax
from jax.experimental import pallas as pl
from jax.experimental.pallas import tpu as pltpu
from jax.sharding import Mesh
from jax.sharding import PartitionSpec as P


SLOTS = 8
OLD = SLOTS - 1
D = 768
HALF = 384
QG = 256
N_CLS = 128
PER = 3
CLS = ("cls_0", "cls_1", "cls_2")
CLS_REP = ("cls_0", "cls_1", "cls_2", "rep")
ROWS = PER * HALF
SEND = ROWS + D
QUARTER = 192
BACK = D + 256
F32 = jnp.float32
BF16 = jnp.bfloat16
PARAMS = pltpu.CompilerParams(vmem_limit_bytes=24 * 1024 * 1024)


def vmem_spec():
    return pl.BlockSpec(memory_space=pltpu.VMEM)


def smem_spec():
    return pl.BlockSpec(memory_space=pltpu.SMEM)


def iota(shape, dim):
    return lax.broadcasted_iota(jnp.int32, shape, dim)


def dot(a, b):
    return jnp.dot(a, b, preferred_element_type=F32)


def dot_last(a, b):
    return lax.dot_general(a, b, (((1,), (1,)), ((), ())), preferred_element_type=F32)


def dot_first(a, b):
    return lax.dot_general(a, b, (((0,), (0,)), ((), ())), preferred_element_type=F32)


def one_hot(mask):
    return jnp.where(mask, 1.0, 0.0).astype(BF16)


def spread_down(row):
    return jnp.broadcast_to(row, (128, 128)).T


def own_target_rows():
    row = 3 * lax.axis_index(CLS_REP)
    return row, pl.multiple_of(jnp.minimum(row // 8 * 8, 768 - 16), 8)


def encode_kernel(
    feat_ref, weight_ref, gain_ref, tgt_ref, q_ref, out_ref, row_ref,
    feat_buf, weight_buf, gain_buf, tgt_buf, q_buf, sems,
):
    row, begin = own_target_rows()
    pairs = [
        (tgt_ref.at[pl.ds(begin, 16), :], tgt_buf), (q_ref, q_buf), (weight_ref, weight_buf),
        (feat_ref, feat_buf), (gain_ref, gain_buf),
    ]
    copies = [pltpu.make_async_copy(a, b, sems.at[i]) for i, (a, b) in enumerate(pairs)]
    for copy in copies:
        copy.start()
    copies[0].wait()
    rows = [tgt_buf[pl.ds(row - begin + a, 1), :].astype(F32) for a in range(3)]
    columns = [spread_down(row) for row in rows]
    ranks = []
    for row in rows:
        rank = jnp.zeros((1, 128), F32)
        for column in columns:
            rank += jnp.sum(jnp.where(column < row, 1.0, 0.0), axis=0, keepdims=True)
        ranks.append(rank)
    rank = jnp.concatenate(ranks, axis=1)
    line = iota((QG, HALF), 0)
    first = ((line >> 1) * PER).astype(F32)
    odd = (line & 1) == 1
    chosen = []
    for k in range(PER):
        hit = rank == first + float(k)
        chosen.append((one_hot(hit & ~odd), one_hot(hit & odd)))
    copies[1].wait()
    out_ref[..., ROWS:] = jnp.broadcast_to(q_buf[...], (N_CLS, 2, D))
    for copy in copies[2:]:
        copy.wait()
    hidden = dot(feat_buf[...], weight_buf[...])
    mean = jnp.mean(hidden * hidden, axis=1, keepdims=True)
    gain = jnp.concatenate([gain_buf[i : i + 1, :] for i in range(6)], axis=1)
    encoded = (hidden * lax.rsqrt(mean + 1e-06) * gain).astype(BF16)
    row_ref[...] = encoded
    for k, (even_rows, odd_rows) in enumerate(chosen):
        total = dot(even_rows, encoded[:, :HALF]) + dot(odd_rows, encoded[:, HALF:])
        out_ref[..., k * HALF : (k + 1) * HALF] = total.astype(BF16).reshape(N_CLS, 2, HALF)


def hits_at(plane_ref, label):
    hits = jnp.zeros((QG, 128), F32)
    for k in range(4):
        hits += jnp.where(plane_ref[k] == label, 1.0, 0.0)
    return hits.astype(BF16)


def hits_of(plane_ref, first):
    return hits_at(plane_ref, iota((QG, 128), 1).astype(F32) + first.astype(F32))


def place_kernel(
    slot_ref, tgt_ref, ids_ref, free_ref, row_ref, key_ref, plane_ref, flag_ref, here_ref,
    there_ref, tgt_buf, ids_buf, free_buf, across_ref, sems,
):
    pairs = [(ids_ref, ids_buf), (tgt_ref, tgt_buf), (free_ref, free_buf)]
    copies = [pltpu.make_async_copy(a, b, sems.at[i]) for i, (a, b) in enumerate(pairs)]
    for copy in copies:
        copy.start()
    cls_index, rep_index = lax.axis_index(CLS), lax.axis_index("rep")
    first = cls_index * (SLOTS * D)
    lane = iota((QG, 128), 1)
    seen = jnp.zeros((QG, 128), F32)
    copies[0].wait()

    def plane_of(half, k):
        own = (ids_buf[half, k : k + 1, :] - first).astype(F32)
        return jnp.concatenate([spread_down(own[:, :128]), spread_down(own[:, 128:])], axis=0)

    for k in range(4):
        across_ref[k] = plane_of(1 - rep_index, k)
        plane = plane_of(rep_index, k)
        plane_ref[k] = plane
        seen = jnp.where((plane.astype(jnp.int32) >> 7) == lane, 1.0, seen)
    flag_ref[...] = jnp.max(seen, axis=0, keepdims=True).astype(jnp.int32)

    copies[1].wait()
    base = cls_index * (2 * HALF) + rep_index * HALF
    parts = [tgt_buf[pl.ds(3 * rep_index + a, N_CLS, stride=6), :] for a in range(3)]
    offsets = jnp.concatenate(parts, axis=1) - base
    inside = (offsets >= 0) & (offsets < HALF)
    far = 4096.0
    keys = jnp.where(inside, offsets.astype(F32), far)
    source = iota((N_CLS, QG), 0)
    twice = (iota((N_CLS, QG), 1) >> 1) == source
    for k in range(PER):
        least = jnp.min(keys, axis=1, keepdims=True)
        keys = jnp.where(keys == least, far, keys)
        wide = jnp.broadcast_to(least, (N_CLS, QG))
        key_ref[k : k + 1, :] = jnp.sum(jnp.where(twice, wide, 0.0), axis=0, keepdims=True)

    slot_first = slot_ref[0] * D
    free_first = slot_first + rep_index * HALF
    labels = []
    for part in range(3):
        target = tgt_buf[pl.ds(3 * lax.axis_index(CLS_REP) + part, 1), :]
        owner = ((target >> 8) * 21846) >> 16
        local = (owner - cls_index) * (SLOTS * D) + slot_first + (target - owner * D)
        labels.append(local.astype(F32))
    copies[2].wait()
    for planes, out_ref in ((across_ref, there_ref), (plane_ref, here_ref)):
        total = jnp.zeros((QG, D), F32)
        for part in range(3):
            rows = slice(part * 128, (part + 1) * 128)
            total += dot(hits_of(planes, free_first + part * 128), free_buf[rows, :])
            total += dot(hits_at(planes, labels[part]), row_ref[rows, :])
        out_ref[...] = total.astype(out_ref.dtype)


def positive_kernel(slot_ref, flag_ref, plane_ref, lab_ref, out_ref, lab_buf, sems):
    out_ref[...] = jnp.zeros_like(out_ref)

    def copy_of(i, part):
        tile = (i + (i >= slot_ref[0]).astype(jnp.int32)) * 6 + part
        at = i * 6 + part
        return tile, pltpu.make_async_copy(
            lab_ref.at[pl.ds(tile * 128, 128), :], lab_buf.at[at], sems.at[at]
        )

    for i in range(OLD):
        for part in range(6):
            tile, copy = copy_of(i, part)
            pl.when(flag_ref[0, tile] > 0)(copy.start)

    def body(at, carry):
        i = at // 6
        tile, copy = copy_of(i, at - i * 6)

        @pl.when(flag_ref[0, tile] > 0)
        def _():
            copy.wait()
            out_ref[...] += dot(hits_of(plane_ref, tile * 128), lab_buf[at])

        return carry

    lax.fori_loop(0, OLD * 6, body, 0)


def quarter_kernel(old_ref, here_ref, came_ref, *out_refs):
    total = (old_ref[...] + here_ref[...] + came_ref[...].astype(F32)).astype(BF16)
    line, lane = iota((D, 256), 0), iota((D, 256), 1)
    for shift, out_ref in enumerate(out_refs):
        first = ((lax.axis_index("cls_2") + shift) & 3) * QUARTER
        pick = one_hot((line == first + lane) & (lane < QUARTER))
        out_ref[...] = dot(total, pick).astype(BF16)


def refresh_kernel(key_ref, got_ref, free_ref, *refs):
    out_ref = refs[-1]
    own = iota((HALF, QG), 0).astype(F32)
    odd = (iota((HALF, QG), 1) & 1) == 1
    matches = [key_ref[k : k + 1, :] == own for k in range(PER)]
    got = [got_ref[..., k * HALF : (k + 1) * HALF].reshape(QG, HALF) for k in range(PER)]
    for h in range(2):
        cols = slice(h * HALF, (h + 1) * HALF)
        mine = odd if h else ~odd
        placed = jnp.zeros((HALF, HALF), F32)
        for k in range(PER):
            placed += dot(one_hot(matches[k] & mine), got[k])
        out_ref[:, cols] = (free_ref[:, cols].astype(F32) + placed).astype(BF16)


def three_parts(value):
    high = value.astype(BF16).astype(F32)
    rest = value - high
    middle = rest.astype(BF16).astype(F32)
    return [high, middle, rest - middle]


def over_lanes(fn, value):
    total = value[:, :128]
    for at in range(128, value.shape[1], 128):
        total = fn(total, value[:, at : at + 128])
    return total


def absorb_all(state, queries, blocks, waits):
    peak, total, grads = state

    def logits_of(i):
        for copy in waits[i]:
            copy.wait()
        return dot_last(queries, blocks[i][...])

    following = logits_of(0)
    for i, block in enumerate(blocks):
        logits = following
        if i + 1 < len(blocks):
            following = logits_of(i + 1)
        higher = jnp.maximum(peak, jnp.max(over_lanes(jnp.maximum, logits), axis=1, keepdims=True))
        scale = jnp.exp(peak - higher)
        weight = jnp.exp(logits - higher)
        total = total * scale + over_lanes(jnp.add, weight)
        grads = grads * scale + dot(weight.astype(BF16), block[...])
        peak = higher
    return peak, total, grads


def old_kernel(
    slot_ref, got_ref, own_ref, lab_ref, out_ref, peak_ref, total_ref, grad_ref, lab_buf, sems
):
    slot = slot_ref[0]
    copies = []
    for i in range(OLD):
        source = (i + (i >= slot).astype(jnp.int32)) * D
        copies.append(
            pltpu.make_async_copy(lab_ref.at[pl.ds(source, D), :], lab_buf.at[i], sems.at[i])
        )
        copies[-1].start()
    out_copy = pltpu.make_async_copy(own_ref, out_ref, sems.at[OLD])
    out_copy.start()
    start = (jnp.full((QG, 1), -jnp.inf, F32), jnp.zeros((QG, 128), F32), jnp.zeros((QG, D), F32))
    peak, total, grads = absorb_all(
        start,
        got_ref[..., ROWS:].reshape(QG, D),
        [own_ref] + [lab_buf.at[i] for i in range(OLD)],
        [[]] + [[copy] for copy in copies],
    )
    peak_ref[...] = jnp.broadcast_to(peak, (QG, 128))
    total_ref[...] = total
    grad_ref[...] = grads
    out_copy.wait()


def score_kernel(
    slot_ref, flag_ref, got_ref, own_ref, other_ref, peak_ref, total_ref, grad_ref, plane_ref,
    pos_ref, *refs
):
    quarter_refs, (out_ref, pos_buf) = refs[:4], refs[4:]
    rep = lax.axis_index("rep")
    slot = slot_ref[0]
    queries = got_ref[..., ROWS:].reshape(QG, D)
    state = (peak_ref[:, :1], total_ref[...], grad_ref[...])
    peak, total, grads = absorb_all(state, queries, [other_ref], [[]])
    out_ref[..., :D] = grads.astype(BF16).reshape(N_CLS, 2, D)
    pos_buf[...] = pos_ref[...]
    for block, half in ((own_ref, rep), (other_ref, 1 - rep)):
        for part in range(3):
            tile = slot * 6 + half * 3 + part

            @pl.when(flag_ref[0, tile] > 0)
            def _():
                rows = block[part * 128 : (part + 1) * 128, :]
                pos_buf[...] += dot(hits_of(plane_ref, tile * 128), rows)

    positive = pos_buf[...]
    picked = jnp.sum(queries.astype(F32) * positive, axis=1, keepdims=True)
    exp_total = jnp.sum(total, axis=1, keepdims=True)
    lane = iota((QG, 256), 1)
    tail = sum(ref[...].astype(F32) for ref in quarter_refs)
    for at, part in enumerate(three_parts(peak) + three_parts(exp_total) + three_parts(picked)):
        tail = jnp.where(lane == QUARTER + at, part, tail)
    out_ref[..., D:] = tail.astype(BF16).reshape(N_CLS, 2, 256)


def finish_kernel(ids_ref, back_ref, loss_ref, grad_ref):
    back = back_ref[...].reshape(QG, BACK)
    tail = back[:, D:].astype(F32)
    stats = tail[:, 128:]

    def column(at):
        at += QUARTER - 128
        return stats[:, at : at + 1] + stats[:, at + 1 : at + 2] + stats[:, at + 2 : at + 3]

    peak, total, picked = column(0), column(3), column(6)
    odd = (iota((QG, 1), 0) & 1) == 1
    ring = (iota((QG, 1), 0) >> 1) & 3
    valid = jnp.where(ids_ref[lax.axis_index("rep")] >= 0, 1.0, 0.0)
    column_of = iota((4, QG), 1) - 2 * lax.axis_index(CLS)
    losses, weights, picks = [], [], []
    for h in range(2):
        mine = odd if h else ~odd
        top = jnp.max(jnp.where(mine, peak, -jnp.inf), axis=0, keepdims=True)
        weight = jnp.where(mine, jnp.exp(peak - top), 0.0)
        exp_total = jnp.sum(weight * total, axis=0, keepdims=True)
        count = jnp.sum(jnp.where(column_of == h, valid, 0.0), axis=1, keepdims=True)
        inverse = 1.0 / jnp.sum(count, axis=0, keepdims=True)
        chosen = jnp.sum(jnp.where(mine, picked, 0.0), axis=0, keepdims=True)
        losses.append(top + jnp.log(exp_total) - chosen * inverse)
        weights.append(weight / exp_total)
        picks.append(inverse)
    loss_ref[...] = jnp.concatenate(losses, axis=1)
    lane = iota((QG, 128), 1)
    table = jnp.where(lane == 8 + 4 * jnp.where(odd, 1, 0) + ring, 1.0, 0.0)
    for h in range(2):
        for at, part in enumerate(three_parts(weights[h])):
            table = jnp.where(lane == 3 * h + at, part, table)
    sums = dot_first(table.astype(BF16), back)
    grads = []
    for h in range(2):
        positive = jnp.concatenate(
            [sums[8 + 4 * h + x : 9 + 4 * h + x, D : D + QUARTER] for x in range(4)], axis=1
        )
        scaled = sums[3 * h : 3 * h + 1, :D] + sums[3 * h + 1 : 3 * h + 2, :D]
        scaled += sums[3 * h + 2 : 3 * h + 3, :D]
        grads.append(scaled - positive * picks[h])
    grad_ref[...] = jnp.concatenate(grads, axis=0).astype(BF16).reshape(1, 2, D)


def in_hbm(value):
    return pltpu.with_memory_space_constraint(value, pltpu.HBM)


def per_device(
    queries,
    positives,
    label_vectors,
    refresh_slot,
    features,
    encoder_weight,
    encoder_gain,
    free_vectors,
    targets,
):
    target_rows = targets.reshape(768, 128)
    label_vectors = in_hbm(label_vectors)
    slot = refresh_slot.reshape(1)
    ids = positives.transpose(0, 2, 1)

    any_spec = pl.BlockSpec(memory_space=pl.ANY)
    sending, encoded = pl.pallas_call(
        encode_kernel,
        out_shape=[
            jax.ShapeDtypeStruct((N_CLS, 2, SEND), BF16),
            jax.ShapeDtypeStruct((HALF, D), BF16),
        ],
        in_specs=[any_spec] * 5,
        out_specs=[vmem_spec()] * 2,
        scratch_shapes=[
            pltpu.VMEM((HALF, D), BF16),
            pltpu.VMEM((D, D), BF16),
            pltpu.VMEM((6, 128), F32),
            pltpu.VMEM((16, 128), jnp.int32),
            pltpu.VMEM((1, 2, D), BF16),
            pltpu.SemaphoreType.DMA((5,)),
        ],
        compiler_params=PARAMS,
        name="encode",
    )(
        in_hbm(features),
        in_hbm(encoder_weight),
        in_hbm(encoder_gain.reshape(6, 128)),
        in_hbm(target_rows),
        in_hbm(queries),
    )
    keys, planes, flags, here, there = pl.pallas_call(
        place_kernel,
        out_shape=[
            jax.ShapeDtypeStruct((8, QG), F32),
            jax.ShapeDtypeStruct((4, QG, 128), F32),
            jax.ShapeDtypeStruct((1, 128), jnp.int32),
            jax.ShapeDtypeStruct((QG, D), F32),
            jax.ShapeDtypeStruct((QG, D), BF16),
        ],
        in_specs=[smem_spec()] + [any_spec] * 3 + [vmem_spec()],
        out_specs=[vmem_spec()] * 5,
        scratch_shapes=[
            pltpu.VMEM((768, 128), jnp.int32),
            pltpu.VMEM((2, 4, QG), jnp.int32),
            pltpu.VMEM((HALF, D), BF16),
            pltpu.VMEM((4, QG, 128), F32),
            pltpu.SemaphoreType.DMA((3,)),
        ],
        compiler_params=PARAMS,
        name="place",
    )(slot, in_hbm(target_rows), in_hbm(ids), in_hbm(free_vectors), encoded)
    got = lax.all_to_all(sending, CLS, 0, 0, tiled=True)

    positive_old = pl.pallas_call(
        positive_kernel,
        out_shape=jax.ShapeDtypeStruct((QG, D), F32),
        in_specs=[smem_spec()] * 2 + [vmem_spec(), any_spec],
        out_specs=vmem_spec(),
        scratch_shapes=[
            pltpu.VMEM((OLD * 6, 128, D), BF16),
            pltpu.SemaphoreType.DMA((OLD * 6,)),
        ],
        compiler_params=PARAMS,
        name="positive",
    )(slot, flags, planes, label_vectors)

    came = lax.ppermute(there, "rep", [(0, 1), (1, 0)])
    quarters = pl.pallas_call(
        quarter_kernel,
        out_shape=[jax.ShapeDtypeStruct((QG, 256), BF16)] * 4,
        in_specs=[vmem_spec()] * 3,
        out_specs=[vmem_spec()] * 4,
        compiler_params=PARAMS,
        name="quarter",
    )(positive_old, here, came)
    along_x = [quarters[0]]
    for shift in (1, 2, 3):
        pairs = [(x, (x + shift) % 4) for x in range(4)]
        along_x.append(lax.ppermute(quarters[shift], "cls_2", pairs))

    own = pl.pallas_call(
        refresh_kernel,
        out_shape=jax.ShapeDtypeStruct((HALF, D), BF16),
        in_specs=[vmem_spec()] * 3 + [any_spec],
        out_specs=vmem_spec(),
        compiler_params=PARAMS,
        name="refresh",
    )(keys, got, free_vectors, quarters[0])
    partner = lax.ppermute(own, "rep", [(0, 1), (1, 0)])

    refreshed, *state = pl.pallas_call(
        old_kernel,
        out_shape=[
            pltpu.HBM((HALF, D), BF16),
            jax.ShapeDtypeStruct((QG, 128), F32),
            jax.ShapeDtypeStruct((QG, 128), F32),
            jax.ShapeDtypeStruct((QG, D), F32),
        ],
        in_specs=[smem_spec(), vmem_spec(), vmem_spec(), any_spec],
        out_specs=[any_spec] + [vmem_spec()] * 3,
        scratch_shapes=[
            pltpu.VMEM((OLD, D, D), BF16),
            pltpu.SemaphoreType.DMA((SLOTS,)),
        ],
        compiler_params=PARAMS,
        name="old",
    )(slot, got, own, label_vectors)
    partner, *state = lax.optimization_barrier((partner, *state))
    leaving = pl.pallas_call(
        score_kernel,
        out_shape=jax.ShapeDtypeStruct((N_CLS, 2, BACK), BF16),
        in_specs=[smem_spec()] * 2 + [vmem_spec()] * 12,
        out_specs=vmem_spec(),
        scratch_shapes=[
            pltpu.VMEM((QG, D), F32),
        ],
        compiler_params=PARAMS,
        name="score",
    )(slot, flags, got, own, partner, *state, planes, positive_old, *along_x)
    back = lax.all_to_all(leaving, CLS, 0, 0, tiled=True)
    loss, grads = pl.pallas_call(
        finish_kernel,
        out_shape=[jax.ShapeDtypeStruct((1, 2), F32), jax.ShapeDtypeStruct((1, 2, D), BF16)],
        in_specs=[vmem_spec()] * 2,
        out_specs=[vmem_spec()] * 2,
        compiler_params=PARAMS,
        name="finish",
    )(ids, back)
    return loss, grads, refreshed


def solution(mesh):
    torus = Mesh(
        mesh.devices.reshape(4, 8, 4, mesh.shape["rep"]), ("cls_0", "cls_1", "cls_2", "rep")
    )
    placed = (
        P("rep", CLS, None),
        P(),
        P(CLS, None),
        P(),
        P(CLS_REP, None),
        P(),
        P(),
        P(CLS_REP, None),
        P(),
    )
    return jax.shard_map(
        per_device,
        mesh=torus,
        in_specs=placed,
        out_specs=(P("rep", CLS), P("rep", CLS, None), P(CLS_REP, None)),
        check_vma=False,
    )
```
